32 devices in a mesh: owner: 8 (over z, y), sub: 4 (over x, core).
Axes of the slice: x: 2, y: 2, z: 4, core: 2. Of those that a mesh axis runs over, the one named last changes fastest.
Arguments:
- velocity: float32 [6, 16384], P(None, 'owner'), may hold values from -6 to 6
- properties: float32 [4, 16384], P(None, 'owner'), may hold values from 0.3 to 3
- first_body: int32 [262144], P(('owner', 'sub')), may hold values from 0 to 16383, as said below
- second_body: int32 [262144], P(('owner', 'sub')), may hold values from 0 to 16383, as said below
- geometry: float32 [9, 262144], P(None, ('owner', 'sub')), may hold values from -2 to 2, as said below
- target_speed: float32 [262144], P(('owner', 'sub')), may hold values from -1 to 2
- warm_impulse: float32 [262144], P(('owner', 'sub')), may hold values from 0 to 0.5
- live_pairs: int32 [2048], P(('owner', 'sub')), may hold values from 0 to 128, as said below
Outputs:
- velocity_out: float32 [6, 16384], P(None, 'owner')
- impulse_out: float32 [262144], P(('owner', 'sub'))
The draws below stay inside these ranges and needn't reach their ends.
Inputs may be any that keep to these rules, and one draw needn't show every extreme that they name: Pair slots are ordered by device of owner+sub, then by partner owner, then by 8 blocks of 128 slots; a slot on a device of owner o with partner owner q has first_body in [o * 2048, (o+1) * 2048) and second_body in [q * 2048, (q+1) * 2048). `second_body`: see first_body. `live_pairs`: on every device the first block toward its own owner is full; live counts differ strongly between devices and between partner owners. `geometry`: rows 0 to 2 of every column have unit length.
All inputs are finite; a program needn't handle non-finite values.
Results may differ from the reference program's by a relative error of at most 0.0001.
Values sent between devices are 32-bit elements; how exact they have to be, the bound alone decides.
A program may use at most 128 MiB of HBM per device.

```python
import math
import jax
import jax.numpy as jnp

B_OWN = 2048
KB = 8
PAIR = 128
ITERS = 4
BODIES = 16384
PAIRS = 262144
BLOCKS = 2048
N_OWNER = 8
N_SUB = 4


def slot_owners():
    slots = jnp.arange(PAIRS, dtype=jnp.int32)
    owner_of = slots // (N_OWNER * KB * PAIR * N_SUB)
    partner = slots // (KB * PAIR) % N_OWNER
    return (owner_of, partner)


def draw_first_body(key, part):
    owner_of, partner = slot_owners()
    return owner_of * B_OWN + jax.random.randint(jax.random.fold_in(key, 11), (PAIRS,), 0, B_OWN, dtype=jnp.int32)


def draw_second_body(key, part):
    owner_of, partner = slot_owners()
    return partner * B_OWN + jax.random.randint(jax.random.fold_in(key, 12), (PAIRS,), 0, B_OWN, dtype=jnp.int32)


def draw_live_pairs(key, part):
    blocks = jnp.arange(BLOCKS, dtype=jnp.int32)
    per_device = N_OWNER * KB
    device = blocks // per_device
    owner_of = device // N_SUB
    partner = blocks // KB % N_OWNER
    apart = jnp.abs(partner - owner_of)
    apart = jnp.minimum(apart, N_OWNER - apart)
    near = (apart <= 1) | (apart == 4)
    level = jax.random.randint(jax.random.fold_in(key, 21), (N_OWNER * N_SUB,), 1, 5, dtype=jnp.int32)[device]
    near_counts = jax.random.randint(jax.random.fold_in(key, 22), (BLOCKS,), PAIR // 2, PAIR + 1, dtype=jnp.int32)
    far_counts = jax.random.randint(jax.random.fold_in(key, 23), (BLOCKS,), 0, PAIR // 4 + 1, dtype=jnp.int32)
    far_counts = jnp.minimum(far_counts * level // 2, PAIR)
    counts = jnp.where(near, near_counts, far_counts)
    own_first = (partner == owner_of) & (blocks % KB == 0)
    return jnp.where(own_first, PAIR, counts).astype(jnp.int32)


def draw_geometry(key, part):
    angle = jax.random.uniform(jax.random.fold_in(key, 31), (PAIRS,), jnp.float32, -3.14159, 3.14159)
    height = jax.random.uniform(jax.random.fold_in(key, 32), (PAIRS,), jnp.float32, -1.0, 1.0)
    radial = jnp.sqrt(jnp.maximum(1.0 - height * height, 0.0))
    normal = jnp.stack([radial * jnp.cos(angle), radial * jnp.sin(angle), height])
    arms = jax.random.uniform(jax.random.fold_in(key, 33), (6, PAIRS), jnp.float32, -1.0, 1.0)
    return jnp.concatenate([normal, arms]).astype(jnp.float32)


def levels(rng, dims, split, low, high):
    gain, own = 1.0, jax.random.fold_in(rng, 6)
    for dim, parts in split:
        draws = jnp.exp(jax.random.uniform(jax.random.fold_in(own, dim), (parts,), jnp.float32, low / len(split), high / len(split)))
        gain = gain * jnp.repeat(draws, dims[dim] // parts).reshape([-1 if axis == dim else 1 for axis in range(len(dims))])
    return gain


def normal_values(rng, dims, width, most, shards=(), held_as=jnp.bfloat16):
    values = jax.random.normal(rng, dims, jnp.float32) * width
    if len(shards) > 0:
        values = levels(rng, dims, shards, -0.22, 0.18) * values
    return jnp.clip(values, min=-most, max=most).astype(held_as)


def setup_inputs(seed: int = 0) -> dict:
    seeds = jax.random.split(jax.random.key(seed), 9)
    return {
        "velocity": normal_values(seeds[0], (6, BODIES), 1.0, 6.0, ((1, 8),), jnp.float32),
        "properties": jnp.clip(jnp.exp(math.log(3.0) - 2.3025851 * jax.random.uniform(seeds[1], (4, BODIES), jnp.float32) ** levels(seeds[1], (4, BODIES), ((1, 8),), -0.2, 0.2)), 0.3, 3.0),
        "first_body": draw_first_body(jax.random.fold_in(seeds[8], 71), 0),
        "second_body": draw_second_body(jax.random.fold_in(seeds[8], 71), 0),
        "geometry": draw_geometry(jax.random.fold_in(seeds[8], 71), 0),
        "target_speed": jnp.clip(-1.0 + 3.0 * jax.random.uniform(seeds[5], (PAIRS,), jnp.float32) ** levels(seeds[5], (PAIRS,), ((0, 32),), -0.2, 0.2), -1.0, 2.0),
        "warm_impulse": jnp.clip(0.5 * jax.random.uniform(seeds[6], (PAIRS,), jnp.float32) ** levels(seeds[6], (PAIRS,), ((0, 32),), -0.2, 0.2), 0.0, 0.5),
        "live_pairs": draw_live_pairs(jax.random.fold_in(seeds[8], 71), 0),
    }


relax = 0.1


def cross_rows(left, right):
    return jnp.stack([left[1] * right[2] - left[2] * right[1],
                      left[2] * right[0] - left[0] * right[2],
                      left[0] * right[1] - left[1] * right[0]])


def reference(velocity, properties, first_body, second_body, geometry, target_speed, warm_impulse, live_pairs):
    slots = jnp.arange(PAIRS, dtype=jnp.int32)
    live = (slots % PAIR) < jnp.repeat(live_pairs, PAIR, total_repeat_length=PAIRS)
    normal = geometry[0:3]
    arm_first = geometry[3:6]
    arm_second = geometry[6:9]
    cross_first = cross_rows(arm_first, normal)
    cross_second = cross_rows(arm_second, normal)
    props_first = properties[:, first_body]
    props_second = properties[:, second_body]
    mass_sum = props_first[0] + props_second[0] + jnp.sum(cross_first * cross_first * props_first[1:4], 0) + jnp.sum(cross_second * cross_second * props_second[1:4], 0)
    speeds = velocity
    impulse = warm_impulse
    for iteration in range(ITERS):
        vel_first = speeds[:, first_body]
        vel_second = speeds[:, second_body]
        relative = vel_first[0:3] + cross_rows(vel_first[3:6], arm_first) - vel_second[0:3] - cross_rows(vel_second[3:6], arm_second)
        normal_speed = jnp.sum(normal * relative, 0)
        change = relax * (target_speed - normal_speed) / mass_sum
        fresh = jnp.where(live, jnp.maximum(impulse + change, 0.0), impulse)
        applied = fresh - impulse
        impulse = fresh
        delta_first = jnp.concatenate([props_first[0] * applied * normal, props_first[1:4] * (applied * cross_first)])
        delta_second = -jnp.concatenate([props_second[0] * applied * normal, props_second[1:4] * (applied * cross_second)])
        total = jnp.zeros(speeds.shape, jnp.float32).at[:, first_body].add(delta_first).at[:, second_body].add(delta_second)
        speeds = speeds + total
    return speeds, impulse
```

```python
import functools

import jax
import jax.numpy as jnp
from jax import lax
from jax.experimental import pallas as pl
from jax.experimental.pallas import tpu as pltpu
from jax.sharding import PartitionSpec as P

ITERS = 4
LANES = 128
SUB = 8
WIDE = 256
VEL = 6
PROPS = 4
MAIL = 8
relax = 0.1
MESH = pl.DeviceIdType.MESH
KEEP_BYTES = 24 * 1024 * 1024


def cross_rows(left, right):
    return [
        left[1] * right[2] - left[2] * right[1],
        left[2] * right[0] - left[0] * right[2],
        left[0] * right[1] - left[1] * right[0],
    ]


def remote(source, target, send_sem, recv_sem, where):
    return pltpu.make_async_remote_copy(
        src_ref=source,
        dst_ref=target,
        send_sem=send_sem,
        recv_sem=recv_sem,
        device_id=where,
        device_id_type=MESH,
    )


def flip(sub, stage):
    step = 2**stage
    return sub + step - 2 * step * ((sub // step) % 2)


def spread(row, height):
    return jnp.broadcast_to(row, (height, LANES))


def kernel(
    groups, subs, height, blocks, keep, relaxed,
    vel_ref, prop_ref, first_ref, second_ref, geo_ref, target_ref, live_ref, imp_ref,
    vel_out, imp_out,
    table, parts, onehot, low_s, chunk_s, jac, gain, tgt, imp, coef, rowbuf, acc,
    mail_out, mail_in, mass_out, mass_in, talk_out, talk_in, red_out, red_in,
    s_mail, r_mail, s_mass, r_mass, s_talk, r_talk, s_red, r_red,
):
    owner, sub = lax.axis_index("owner"), lax.axis_index("sub")
    stages = subs.bit_length() - 1
    rows = VEL * height
    owned = height * WIDE

    def partner(k):
        return lax.rem(owner + k, groups)

    def there(k):
        return lax.rem(groups - k, groups)

    barrier = pltpu.get_barrier_semaphore()

    def signal(k, carry):
        pl.semaphore_signal(
            barrier, inc=1, device_id=(partner(k), sub), device_id_type=MESH
        )
        return carry

    lax.fori_loop(1, groups, signal, 0)
    for stage in range(stages):
        pl.semaphore_signal(
            barrier, inc=1, device_id=(owner, flip(sub, stage)), device_id_type=MESH
        )

    def mail(k):
        return remote(
            mail_out.at[k], mail_in.at[there(k)], s_mail.at[k], r_mail.at[there(k)],
            (partner(k), sub),
        )

    def mail_here(k):
        return remote(
            mail_out.at[k], mail_in.at[k], s_mail.at[k], r_mail.at[k], (partner(k), sub)
        )

    def mass(k):
        return remote(
            mass_out.at[k], mass_in.at[there(k)], s_mass.at[k], r_mass.at[there(k)],
            (partner(k), sub),
        )

    def mass_here(k):
        return remote(
            mass_out.at[k], mass_in.at[k], s_mass.at[k], r_mass.at[k], (partner(k), sub)
        )

    def talk(t, k):
        return remote(
            talk_out.at[t, k], talk_in.at[t, there(k)], s_talk.at[t, k],
            r_talk.at[t, there(k)], (partner(k), sub),
        )

    def talk_here(t, k):
        return remote(
            talk_out.at[t, k], talk_in.at[t, k], s_talk.at[t, k], r_talk.at[t, k],
            (partner(k), sub),
        )

    def part(b):
        return pl.ds(b * SUB, SUB)

    def over_blocks(body):
        if blocks == 1:
            body(0)
        else:
            def run(b, carry):
                body(b)
                return carry

            lax.fori_loop(0, blocks, run, 0)

    def live_of(q, b):
        lane = lax.broadcasted_iota(jnp.int32, (SUB, LANES), 1)
        return lane < live_ref[q, part(b)]

    def local(index):
        return index - lax.div(index, jnp.full_like(index, owned)) * owned

    def write_mail(k):
        q = partner(k)

        def block(b):
            normal = [geo_ref[r, q, part(b)] for r in range(3)]
            cross = cross_rows([geo_ref[6 + r, q, part(b)] for r in range(3)], normal)
            live = live_of(q, b)
            for r, value in enumerate(normal + cross):
                mail_out[k, r, part(b)] = jnp.where(live, -value, 0.0)
            mail_out[k, VEL, part(b)] = local(second_ref[q, part(b)]).astype(jnp.float32)
            mail_out[k, VEL + 1, part(b)] = imp_ref[q, part(b)]

        over_blocks(block)

    def post(k, carry):
        write_mail(k)
        mail(k).start()
        return carry

    pl.semaphore_wait(barrier, groups - 1 + stages)
    lax.fori_loop(1, groups, post, 0)
    write_mail(0)

    for r in range(VEL):
        for c in range(height):
            table[pl.ds(r * height + c, 1), :] = vel_ref[pl.ds(r, 1), pl.ds(c * WIDE, WIDE)]
    for r in range(PROPS):
        for c in range(height):
            rowbuf[pl.ds(r * height + c, 1), :] = prop_ref[pl.ds(r, 1), pl.ds(c * WIDE, WIDE)]
    prop_value = rowbuf[pl.ds(0, PROPS * height), :]
    prop_high = prop_value.astype(jnp.bfloat16)
    prop_rest = prop_value - prop_high.astype(jnp.float32)
    parts[0, pl.ds(0, PROPS * height), :] = prop_high
    parts[1, pl.ds(0, PROPS * height), :] = prop_rest.astype(jnp.bfloat16)

    def hot(low, i):
        tall = lax.broadcasted_iota(jnp.int32, (WIDE, LANES), 0)
        return jnp.where(tall == spread(low[i : i + 1], WIDE), 1.0, 0.0).astype(jnp.bfloat16)

    def hot_tile(side, k, b):
        if keep:
            return onehot[side, k, b]
        low = low_s[side, k, part(b)]
        return jnp.concatenate([hot(low, i) for i in range(SUB)], axis=1)

    def hits(side, k, b):
        tall = lax.broadcasted_iota(jnp.int32, (height, LANES), 0)
        chunk = chunk_s[side, k, part(b)]
        return [tall == spread(chunk[i : i + 1], height) for i in range(SUB)]

    def picked(count, side, k, b):
        tile = hot_tile(side, k, b)
        high = parts[0, pl.ds(0, count * height), :]
        rest = parts[1, pl.ds(0, count * height), :]
        return jnp.dot(high, tile, preferred_element_type=jnp.float32) + jnp.dot(
            rest, tile, preferred_element_type=jnp.float32
        )

    def prepare(side, k, b, index, values):
        low_s[side, k, part(b)] = lax.rem(index, jnp.full_like(index, WIDE))
        chunk_s[side, k, part(b)] = lax.div(index, jnp.full_like(index, WIDE))
        low = low_s[side, k, part(b)]
        if keep:
            for i in range(SUB):
                onehot[side, k, b, :, pl.ds(i * LANES, LANES)] = hot(low, i)
        got = picked(PROPS, side, k, b)
        masks = hits(side, k, b)
        prop = []
        for r in range(PROPS):
            found = []
            for i in range(SUB):
                piece = got[r * height : (r + 1) * height, i * LANES : (i + 1) * LANES]
                found.append(jnp.sum(jnp.where(masks[i], piece, 0.0), axis=0, keepdims=True))
            prop.append(jnp.concatenate(found, axis=0))
        total = prop[0]
        for r in range(VEL):
            jac[side, k, r, part(b)] = values[r]
            gain[side, k, r, part(b)] = prop[max(0, r - 2)] * values[r]
        for r in range(3):
            total += values[3 + r] * values[3 + r] * prop[1 + r]
        mass_out[k, side, part(b)] = total

    def prepare_first(k, carry):
        q = partner(k)

        def block(b):
            normal = [geo_ref[r, q, part(b)] for r in range(3)]
            cross = cross_rows([geo_ref[3 + r, q, part(b)] for r in range(3)], normal)
            prepare(0, k, b, local(first_ref[q, part(b)]), normal + cross)
            tgt[0, k, part(b)] = target_ref[q, part(b)]
            imp[0, k, part(b)] = imp_ref[q, part(b)]

        over_blocks(block)
        return carry

    def prepare_second(source, k):
        def block(b):
            values = [source[k, r, part(b)] for r in range(VEL)]
            prepare(1, k, b, source[k, VEL, part(b)].astype(jnp.int32), values)
            tgt[1, k, part(b)] = jnp.zeros((SUB, LANES), jnp.float32)
            imp[1, k, part(b)] = source[k, VEL + 1, part(b)]

        over_blocks(block)

    lax.fori_loop(0, groups, prepare_first, 0)
    prepare_second(mail_out, 0)

    def receive(k, carry):
        mail_here(k).wait_recv()
        prepare_second(mail_in, k)
        mass(k).start()
        return carry

    lax.fori_loop(1, groups, receive, 0)

    def coefficients(side, k, b, peer):
        value = relaxed / (mass_out[k, side, part(b)] + peer)
        if side == 0:
            value = jnp.where(live_of(partner(k), b), value, 0.0)
        coef[side, k, part(b)] = value

    def settle(k, carry):
        mass_here(k).wait_recv()

        def block(b):
            for side in range(2):
                coefficients(side, k, b, mass_in[k, 1 - side, part(b)])

        over_blocks(block)
        return carry

    def settle_own(b):
        for side in range(2):
            coefficients(side, 0, b, mass_out[0, 1 - side, part(b)])

    def speak(t, k):
        def block(b):
            for side in range(2):
                got = picked(VEL, side, k, b)
                masks = hits(side, k, b)
                found = []
                for i in range(SUB):
                    total = jnp.zeros((height, LANES), jnp.float32)
                    for r in range(VEL):
                        piece = got[r * height : (r + 1) * height, i * LANES : (i + 1) * LANES]
                        line = jac[side, k, r, pl.ds(b * SUB + i, 1)]
                        total += piece * spread(line, height)
                    found.append(
                        jnp.sum(jnp.where(masks[i], total, 0.0), axis=0, keepdims=True)
                    )
                talk_out[t, k, side, part(b)] = tgt[side, k, part(b)] - jnp.concatenate(
                    found, axis=0
                )

        over_blocks(block)

    def place(deltas, side, k, b):
        coarse = [d.astype(jnp.bfloat16).astype(jnp.float32) for d in deltas]
        fine = [d - c for d, c in zip(deltas, coarse)]
        masks = hits(side, k, b)
        left = []
        for i in range(SUB):
            lines = [
                jnp.where(masks[i], spread(x[i : i + 1], height), 0.0) for x in coarse + fine
            ]
            left.append(jnp.concatenate(lines, axis=0).astype(jnp.bfloat16))
        out = lax.dot_general(
            jnp.concatenate(left, axis=1),
            hot_tile(side, k, b),
            (((1,), (1,)), ((), ())),
            preferred_element_type=jnp.float32,
        )
        return out[:rows] + out[rows:]

    def act(t, k, peer_ref):
        def block(b):
            for side in range(2):
                push = talk_out[t, k, side, part(b)] + peer_ref[t, k, 1 - side, part(b)]
                before = imp[side, k, part(b)]
                fresh = jnp.maximum(before + push * coef[side, k, part(b)], 0.0)
                imp[side, k, part(b)] = fresh
                applied = fresh - before
                deltas = [applied * gain[side, k, r, part(b)] for r in range(VEL)]
                acc[...] += place(deltas, side, k, b)

        over_blocks(block)

    def reduce(t, stage):
        return remote(
            red_out.at[t, stage], red_in.at[t, stage], s_red.at[t, stage],
            r_red.at[t, stage], (owner, flip(sub, stage)),
        )

    def iteration(t, carry):
        value = table[...]
        high = value.astype(jnp.bfloat16)
        parts[0] = high
        parts[1] = (value - high.astype(jnp.float32)).astype(jnp.bfloat16)

        def send(k, carry):
            speak(t, k)
            talk(t, k).start()
            return carry

        lax.fori_loop(1, groups, send, 0)
        speak(t, 0)

        @pl.when(t == 0)
        def _():
            over_blocks(settle_own)
            lax.fori_loop(1, groups, settle, 0)

        acc[...] = jnp.zeros_like(acc)
        act(t, 0, talk_out)

        def listen(k, carry):
            talk_here(t, k).wait_recv()
            act(t, k, talk_in)
            return carry

        lax.fori_loop(1, groups, listen, 0)
        total = acc[...]
        for stage in range(stages):
            red_out[t, stage] = total
            reduce(t, stage).start()
            reduce(t, stage).wait_recv()
            total = total + red_in[t, stage]
        table[...] += total
        return carry

    lax.fori_loop(0, ITERS, iteration, 0)

    for r in range(VEL):
        for c in range(height):
            vel_out[pl.ds(r, 1), pl.ds(c * WIDE, WIDE)] = table[pl.ds(r * height + c, 1), :]

    def finish(k, carry):
        imp_out[partner(k)] = imp[0, k]
        return carry

    lax.fori_loop(0, groups, finish, 0)

    def sent(k, carry):
        mail(k).wait_send()
        mass(k).wait_send()
        for t in range(ITERS):
            talk(t, k).wait_send()
        return carry

    lax.fori_loop(1, groups, sent, 0)
    for t in range(ITERS):
        for stage in range(stages):
            reduce(t, stage).wait_send()


def on_device(
    groups, subs, velocity, properties, first_body, second_body, geometry, target_speed,
    warm_impulse, live_pairs
):
    owned = velocity.shape[1]
    height = owned // WIDE
    count = first_body.shape[0]
    rows = count // (groups * LANES)
    blocks = rows // SUB
    tiles = (groups, rows, LANES)
    stages = subs.bit_length() - 1
    keep = 2 * count * WIDE * 2 <= KEEP_BYTES
    kept = (2, groups, blocks, WIDE, SUB * LANES) if keep else (1, 1, 1, 16, LANES)

    rows_per_block = count // live_pairs.shape[0] // LANES
    offset = jnp.arange(count // LANES, dtype=jnp.int32) % rows_per_block * LANES
    bound = jnp.repeat(live_pairs, rows_per_block, total_repeat_length=count // LANES) - offset
    live = jnp.broadcast_to(bound[:, None], (count // LANES, LANES)).reshape(tiles)

    f32 = jnp.float32
    pair = (2, groups, rows, LANES)
    speeds, impulse = pl.pallas_call(
        functools.partial(kernel, groups, subs, height, blocks, keep, relax),
        name="contacts",
        out_shape=(
            jax.ShapeDtypeStruct((VEL, owned), f32),
            jax.ShapeDtypeStruct(tiles, f32),
        ),
        in_specs=[pl.BlockSpec(memory_space=pltpu.VMEM)] * 8,
        out_specs=(pl.BlockSpec(memory_space=pltpu.VMEM),) * 2,
        scratch_shapes=[
            pltpu.VMEM((VEL * height, WIDE), f32),
            pltpu.VMEM((2, VEL * height, WIDE), jnp.bfloat16),
            pltpu.VMEM(kept, jnp.bfloat16),
            pltpu.VMEM(pair, jnp.int32),
            pltpu.VMEM(pair, jnp.int32),
            pltpu.VMEM((2, groups, VEL, rows, LANES), f32),
            pltpu.VMEM((2, groups, VEL, rows, LANES), f32),
            pltpu.VMEM(pair, f32),
            pltpu.VMEM(pair, f32),
            pltpu.VMEM(pair, f32),
            pltpu.VMEM((VEL * height, WIDE), f32),
            pltpu.VMEM((VEL * height, WIDE), f32),
            pltpu.VMEM((groups, MAIL, rows, LANES), f32),
            pltpu.VMEM((groups, MAIL, rows, LANES), f32),
            pltpu.VMEM((groups, 2, rows, LANES), f32),
            pltpu.VMEM((groups, 2, rows, LANES), f32),
            pltpu.VMEM((ITERS, groups, 2, rows, LANES), f32),
            pltpu.VMEM((ITERS, groups, 2, rows, LANES), f32),
            pltpu.VMEM((ITERS, stages, VEL * height, WIDE), f32),
            pltpu.VMEM((ITERS, stages, VEL * height, WIDE), f32),
        ]
        + [pltpu.SemaphoreType.DMA((groups,))] * 4
        + [pltpu.SemaphoreType.DMA((ITERS, groups))] * 2
        + [pltpu.SemaphoreType.DMA((ITERS, stages))] * 2,
        compiler_params=pltpu.CompilerParams(collective_id=0, has_side_effects=True),
    )(
        velocity,
        properties,
        first_body.reshape(tiles),
        second_body.reshape(tiles),
        geometry.reshape((geometry.shape[0],) + tiles),
        target_speed.reshape(tiles),
        live,
        warm_impulse.reshape(tiles),
    )
    return (speeds, impulse.reshape(count))


def solution(mesh):
    groups, subs = mesh.shape["owner"], mesh.shape["sub"]
    return jax.shard_map(
        functools.partial(on_device, groups, subs),
        mesh=mesh,
        in_specs=(
            P(None, "owner"),
            P(None, "owner"),
            P(("owner", "sub")),
            P(("owner", "sub")),
            P(None, ("owner", "sub")),
            P(("owner", "sub")),
            P(("owner", "sub")),
            P(("owner", "sub")),
        ),
        out_specs=(P(None, "owner"), P(("owner", "sub"))),
        check_vma=False,
    )
```

```python
import functools

import jax
import jax.numpy as jnp
from jax import lax
from jax.experimental import pallas as pl
from jax.experimental.pallas import tpu as pltpu
from jax.sharding import PartitionSpec as P

ITERS = 4
LANES = 128
SUB = 8
WIDE = 256
VEL = 6
PROPS = 4
MAIL = 8
relax = 0.1
MESH = pl.DeviceIdType.MESH
KEEP_BYTES = 24 * 1024 * 1024
HOT = jnp.float8_e4m3fn
PAIRED = 2


def cross_rows(left, right):
    return [
        left[1] * right[2] - left[2] * right[1],
        left[2] * right[0] - left[0] * right[2],
        left[0] * right[1] - left[1] * right[0],
    ]


def remote(source, target, send_sem, recv_sem, where):
    return pltpu.make_async_remote_copy(
        src_ref=source,
        dst_ref=target,
        send_sem=send_sem,
        recv_sem=recv_sem,
        device_id=where,
        device_id_type=MESH,
    )


def flip(sub, stage):
    step = 2**stage
    return sub + step - 2 * step * ((sub // step) % 2)


def spread(row, height):
    return jnp.broadcast_to(row, (height, LANES))


def kernel(
    groups, subs, height, blocks, span, keep, relaxed,
    vel_ref, prop_ref, first_ref, second_ref, raw_ref, target_ref, live_ref, imp_ref,
    vel_out, imp_out,
    geo_ref, table, parts, onehot, low_s, chunk_s, jac, gain, tgt, imp, coef, rowbuf, acc,
    mail_out, mail_in, mass_out, mass_in, talk_out, talk_in, red_out, red_in,
    s_mail, r_mail, s_mass, r_mass, s_talk, r_talk, s_red, r_red,
):
    owner, sub = lax.axis_index("owner"), lax.axis_index("sub")
    stages = subs.bit_length() - 1
    rows = VEL * height
    owned = height * WIDE
    full = (groups - 1) // PAIRED
    head = groups - PAIRED * full

    def partner(k):
        return lax.rem(owner + k, groups)

    def there(k):
        return lax.rem(groups - k, groups)

    barrier = pltpu.get_barrier_semaphore()

    def signal(k, carry):
        pl.semaphore_signal(
            barrier, inc=1, device_id=(partner(k), sub), device_id_type=MESH
        )
        return carry

    lax.fori_loop(1, groups, signal, 0)
    for stage in range(stages):
        pl.semaphore_signal(
            barrier, inc=1, device_id=(owner, flip(sub, stage)), device_id_type=MESH
        )

    def mail(k):
        return remote(
            mail_out.at[k], mail_in.at[there(k)], s_mail.at[k], r_mail.at[there(k)],
            (partner(k), sub),
        )

    def mail_here(k):
        return remote(
            mail_out.at[k], mail_in.at[k], s_mail.at[k], r_mail.at[k], (partner(k), sub)
        )

    def mass(k):
        return remote(
            mass_out.at[k], mass_in.at[there(k)], s_mass.at[k], r_mass.at[there(k)],
            (partner(k), sub),
        )

    def mass_here(k):
        return remote(
            mass_out.at[k], mass_in.at[k], s_mass.at[k], r_mass.at[k], (partner(k), sub)
        )

    def talk(t, k):
        return remote(
            talk_out.at[t, k], talk_in.at[t, there(k)], s_talk.at[t, k],
            r_talk.at[t, there(k)], (partner(k), sub),
        )

    def talk_here(t, k):
        return remote(
            talk_out.at[t, k], talk_in.at[t, k], s_talk.at[t, k], r_talk.at[t, k],
            (partner(k), sub),
        )

    def part(b):
        return pl.ds(b * SUB, SUB)

    def over_blocks(body):
        if blocks == 1:
            body(0)
        else:
            def run(b, carry):
                body(b)
                return carry

            lax.fori_loop(0, blocks, run, 0)

    def live_of(q, b):
        lane = lax.broadcasted_iota(jnp.int32, (SUB, LANES), 1)
        line = lax.broadcasted_iota(jnp.int32, (SUB, LANES), 0)
        bound = jnp.zeros((SUB, LANES), jnp.int32)
        for i in range(SUB):
            row = (q * blocks + b) * SUB + i
            left = live_ref[row // span] - (row % span) * LANES
            bound = jnp.where(line == i, left, bound)
        return lane < bound

    def local(index):
        return index - lax.div(index, jnp.full_like(index, owned)) * owned

    def write_mail(k):
        q = partner(k)

        def block(b):
            for r in range(9):
                for i in range(SUB):
                    start = pl.multiple_of(((q * blocks + b) * SUB + i) * LANES, LANES)
                    geo_ref[r, k, pl.ds(b * SUB + i, 1), :] = raw_ref[
                        pl.ds(r, 1), pl.ds(start, LANES)
                    ]
            normal = [geo_ref[r, k, part(b)] for r in range(3)]
            cross = cross_rows([geo_ref[6 + r, k, part(b)] for r in range(3)], normal)
            live = live_of(q, b)
            for r, value in enumerate(normal + cross):
                mail_out[k, r, part(b)] = jnp.where(live, -value, 0.0)
            mail_out[k, VEL, part(b)] = local(second_ref[q, part(b)]).astype(jnp.float32)
            mail_out[k, VEL + 1, part(b)] = imp_ref[q, part(b)]

        over_blocks(block)

    def write(k, carry):
        write_mail(k)
        return carry

    def post(k, carry):
        mail(k).start()
        return carry

    lax.fori_loop(0, groups, write, 0)
    pl.semaphore_wait(barrier, groups - 1 + stages)
    lax.fori_loop(1, groups, post, 0)

    for r in range(VEL):
        for c in range(height):
            table[pl.ds(r * height + c, 1), :] = vel_ref[pl.ds(r, 1), pl.ds(c * WIDE, WIDE)]
    for r in range(PROPS):
        for c in range(height):
            rowbuf[pl.ds(r * height + c, 1), :] = prop_ref[pl.ds(r, 1), pl.ds(c * WIDE, WIDE)]
    prop_value = rowbuf[pl.ds(0, PROPS * height), :]
    prop_high = prop_value.astype(jnp.bfloat16)
    prop_rest = prop_value - prop_high.astype(jnp.float32)
    parts[pl.ds(0, PROPS * height), :] = prop_high
    parts[pl.ds(PROPS * height, PROPS * height), :] = prop_rest.astype(jnp.bfloat16)

    def hot(low, i):
        tall = lax.broadcasted_iota(jnp.int32, (WIDE, LANES), 0)
        return jnp.where(tall == spread(low[i : i + 1], WIDE), 1.0, 0.0).astype(HOT)

    def hot_tile(side, k, b):
        if keep:
            return onehot[side, k, b]
        low = low_s[side, k, part(b)]
        return jnp.concatenate([hot(low, i) for i in range(SUB)], axis=1)

    def hits(side, k, b):
        tall = lax.broadcasted_iota(jnp.int32, (height, LANES), 0)
        chunk = chunk_s[side, k, part(b)]
        return [tall == spread(chunk[i : i + 1], height) for i in range(SUB)]

    def picked(count, side, k, b):
        tile = hot_tile(side, k, b)
        half = count * height
        both = parts[pl.ds(0, 2 * half), :]
        out = lax.dot_general(
            both, tile, (((1,), (0,)), ((), ())), preferred_element_type=jnp.float32
        )
        return out[:half] + out[half:]

    def prepare(side, k, b, index, values):
        low_s[side, k, part(b)] = lax.rem(index, jnp.full_like(index, WIDE))
        chunk_s[side, k, part(b)] = lax.div(index, jnp.full_like(index, WIDE))
        low = low_s[side, k, part(b)]
        if keep:
            for i in range(SUB):
                onehot[side, k, b, :, pl.ds(i * LANES, LANES)] = hot(low, i)
        got = picked(PROPS, side, k, b)
        masks = hits(side, k, b)
        prop = []
        for r in range(PROPS):
            found = []
            for i in range(SUB):
                piece = got[r * height : (r + 1) * height, i * LANES : (i + 1) * LANES]
                found.append(jnp.sum(jnp.where(masks[i], piece, 0.0), axis=0, keepdims=True))
            prop.append(jnp.concatenate(found, axis=0))
        total = prop[0]
        for r in range(VEL):
            jac[side, k, r, part(b)] = values[r]
            gain[side, k, r, part(b)] = prop[max(0, r - 2)] * values[r]
        for r in range(3):
            total += values[3 + r] * values[3 + r] * prop[1 + r]
        mass_out[k, side, part(b)] = total

    def prepare_first(k, carry):
        q = partner(k)

        def block(b):
            normal = [geo_ref[r, k, part(b)] for r in range(3)]
            cross = cross_rows([geo_ref[3 + r, k, part(b)] for r in range(3)], normal)
            prepare(0, k, b, local(first_ref[q, part(b)]), normal + cross)
            tgt[0, k, part(b)] = target_ref[q, part(b)]
            imp[0, k, part(b)] = imp_ref[q, part(b)]

        over_blocks(block)
        return carry

    def prepare_second(source, k):
        def block(b):
            values = [source[k, r, part(b)] for r in range(VEL)]
            prepare(1, k, b, source[k, VEL, part(b)].astype(jnp.int32), values)
            tgt[1, k, part(b)] = jnp.zeros((SUB, LANES), jnp.float32)
            imp[1, k, part(b)] = source[k, VEL + 1, part(b)]

        over_blocks(block)

    lax.fori_loop(0, groups, prepare_first, 0)
    prepare_second(mail_out, 0)

    def receive(k, carry):
        mail_here(k).wait_recv()
        prepare_second(mail_in, k)
        mass(k).start()
        return carry

    lax.fori_loop(1, groups, receive, 0)

    def coefficients(side, k, b, peer):
        value = relaxed / (mass_out[k, side, part(b)] + peer)
        if side == 0:
            value = jnp.where(live_of(partner(k), b), value, 0.0)
        coef[side, k, part(b)] = value

    def settle(k, carry):
        mass_here(k).wait_recv()

        def block(b):
            for side in range(2):
                coefficients(side, k, b, mass_in[k, 1 - side, part(b)])

        over_blocks(block)
        return carry

    def settle_own(b):
        for side in range(2):
            coefficients(side, 0, b, mass_out[0, 1 - side, part(b)])

    def speak(t, ks):
        def block(b):
            for k, side in [(k, side) for k in ks for side in range(2)]:
                got = picked(VEL, side, k, b)
                masks = hits(side, k, b)
                found = []
                for i in range(SUB):
                    total = jnp.zeros((height, LANES), jnp.float32)
                    for r in range(VEL):
                        piece = got[r * height : (r + 1) * height, i * LANES : (i + 1) * LANES]
                        line = jac[side, k, r, pl.ds(b * SUB + i, 1)]
                        total += piece * spread(line, height)
                    found.append(
                        jnp.sum(jnp.where(masks[i], total, 0.0), axis=0, keepdims=True)
                    )
                talk_out[t, k, side, part(b)] = tgt[side, k, part(b)] - jnp.concatenate(
                    found, axis=0
                )

        over_blocks(block)

    def place(deltas, side, k, b):
        coarse = [d.astype(jnp.bfloat16).astype(jnp.float32) for d in deltas]
        fine = [d - c for d, c in zip(deltas, coarse)]
        masks = hits(side, k, b)
        left = []
        for i in range(SUB):
            lines = [
                jnp.where(masks[i], spread(x[i : i + 1], height), 0.0) for x in coarse + fine
            ]
            left.append(jnp.concatenate(lines, axis=0).astype(jnp.bfloat16))
        out = lax.dot_general(
            jnp.concatenate(left, axis=1),
            hot_tile(side, k, b),
            (((1,), (1,)), ((), ())),
            preferred_element_type=jnp.float32,
        )
        return out[:rows] + out[rows:]

    def act(t, ks):
        def block(b):
            moved = []
            for k, side in [(k, side) for k in ks for side in range(2)]:
                peer_ref = talk_out if isinstance(k, int) and k == 0 else talk_in
                push = talk_out[t, k, side, part(b)] + peer_ref[t, k, 1 - side, part(b)]
                before = imp[side, k, part(b)]
                fresh = jnp.maximum(before + push * coef[side, k, part(b)], 0.0)
                imp[side, k, part(b)] = fresh
                applied = fresh - before
                deltas = [applied * gain[side, k, r, part(b)] for r in range(VEL)]
                moved.append(place(deltas, side, k, b))
            acc[...] += functools.reduce(jnp.add, moved)

        over_blocks(block)

    def reduce(t, stage):
        return remote(
            red_out.at[t, stage], red_in.at[t, stage], s_red.at[t, stage],
            r_red.at[t, stage], (owner, flip(sub, stage)),
        )

    def iteration(t, carry):
        value = table[...]
        high = value.astype(jnp.bfloat16)
        parts[pl.ds(0, rows), :] = high
        parts[pl.ds(rows, rows), :] = (value - high.astype(jnp.float32)).astype(jnp.bfloat16)

        def send(ks):
            speak(t, ks)
            for k in ks:
                if not (isinstance(k, int) and k == 0):
                    talk(t, k).start()

        def send_some(j, carry):
            send([1 + PAIRED * j + n for n in range(PAIRED)])
            return carry

        lax.fori_loop(0, full, send_some, 0)
        send(list(range(1 + PAIRED * full, groups)) + [0])

        @pl.when(t == 0)
        def _():
            over_blocks(settle_own)
            lax.fori_loop(1, groups, settle, 0)

        acc[...] = jnp.zeros_like(acc)
        def listen(ks):
            for k in ks:
                if not (isinstance(k, int) and k == 0):
                    talk_here(t, k).wait_recv()
            act(t, ks)

        def listen_some(j, carry):
            listen([head + PAIRED * j + n for n in range(PAIRED)])
            return carry

        listen(list(range(head)))
        lax.fori_loop(0, full, listen_some, 0)
        total = acc[...]
        for stage in range(stages):
            red_out[t, stage] = total
            reduce(t, stage).start()
            reduce(t, stage).wait_recv()
            total = total + red_in[t, stage]
        table[...] += total
        return carry

    lax.fori_loop(0, ITERS, iteration, 0)

    for r in range(VEL):
        for c in range(height):
            vel_out[pl.ds(r, 1), pl.ds(c * WIDE, WIDE)] = table[pl.ds(r * height + c, 1), :]

    def finish(k, carry):
        imp_out[partner(k)] = imp[0, k]
        return carry

    lax.fori_loop(0, groups, finish, 0)

    def sent(k, carry):
        mail(k).wait_send()
        mass(k).wait_send()
        for t in range(ITERS):
            talk(t, k).wait_send()
        return carry

    lax.fori_loop(1, groups, sent, 0)
    for t in range(ITERS):
        for stage in range(stages):
            reduce(t, stage).wait_send()


def on_device(
    groups, subs, velocity, properties, first_body, second_body, geometry, target_speed,
    warm_impulse, live_pairs
):
    owned = velocity.shape[1]
    height = owned // WIDE
    count = first_body.shape[0]
    rows = count // (groups * LANES)
    blocks = rows // SUB
    tiles = (groups, rows, LANES)
    stages = subs.bit_length() - 1
    keep = 2 * count * WIDE <= KEEP_BYTES
    kept = (2, groups, blocks, WIDE, SUB * LANES) if keep else (1, 1, 1, 32, LANES)

    rows_per_block = count // live_pairs.shape[0] // LANES
    f32 = jnp.float32
    pair = (2, groups, rows, LANES)
    speeds, impulse = pl.pallas_call(
        functools.partial(kernel, groups, subs, height, blocks, rows_per_block, keep, relax),
        name="contacts",
        out_shape=(
            jax.ShapeDtypeStruct((VEL, owned), f32),
            jax.ShapeDtypeStruct(tiles, f32),
        ),
        in_specs=[pl.BlockSpec(memory_space=pltpu.VMEM)] * 6
        + [pl.BlockSpec(memory_space=pltpu.SMEM)]
        + [pl.BlockSpec(memory_space=pltpu.VMEM)],
        out_specs=(pl.BlockSpec(memory_space=pltpu.VMEM),) * 2,
        scratch_shapes=[
            pltpu.VMEM((geometry.shape[0],) + tiles, f32),
            pltpu.VMEM((VEL * height, WIDE), f32),
            pltpu.VMEM((2 * VEL * height, WIDE), jnp.bfloat16),
            pltpu.VMEM(kept, HOT),
            pltpu.VMEM(pair, jnp.int32),
            pltpu.VMEM(pair, jnp.int32),
            pltpu.VMEM((2, groups, VEL, rows, LANES), f32),
            pltpu.VMEM((2, groups, VEL, rows, LANES), f32),
            pltpu.VMEM(pair, f32),
            pltpu.VMEM(pair, f32),
            pltpu.VMEM(pair, f32),
            pltpu.VMEM((VEL * height, WIDE), f32),
            pltpu.VMEM((VEL * height, WIDE), f32),
            pltpu.VMEM((groups, MAIL, rows, LANES), f32),
            pltpu.VMEM((groups, MAIL, rows, LANES), f32),
            pltpu.VMEM((groups, 2, rows, LANES), f32),
            pltpu.VMEM((groups, 2, rows, LANES), f32),
            pltpu.VMEM((ITERS, groups, 2, rows, LANES), f32),
            pltpu.VMEM((ITERS, groups, 2, rows, LANES), f32),
            pltpu.VMEM((ITERS, stages, VEL * height, WIDE), f32),
            pltpu.VMEM((ITERS, stages, VEL * height, WIDE), f32),
        ]
        + [pltpu.SemaphoreType.DMA((groups,))] * 4
        + [pltpu.SemaphoreType.DMA((ITERS, groups))] * 2
        + [pltpu.SemaphoreType.DMA((ITERS, stages))] * 2,
        compiler_params=pltpu.CompilerParams(collective_id=0, has_side_effects=True),
    )(
        velocity,
        properties,
        first_body.reshape(tiles),
        second_body.reshape(tiles),
        geometry,
        target_speed.reshape(tiles),
        live_pairs,
        warm_impulse.reshape(tiles),
    )
    return (speeds, impulse.reshape(count))


def solution(mesh):
    groups, subs = mesh.shape["owner"], mesh.shape["sub"]
    return jax.shard_map(
        functools.partial(on_device, groups, subs),
        mesh=mesh,
        in_specs=(
            P(None, "owner"),
            P(None, "owner"),
            P(("owner", "sub")),
            P(("owner", "sub")),
            P(None, ("owner", "sub")),
            P(("owner", "sub")),
            P(("owner", "sub")),
            P(("owner", "sub")),
        ),
        out_specs=(P(None, "owner"), P(("owner", "sub"))),
        check_vma=False,
    )
```

```python
import functools

import jax
import jax.numpy as jnp
from jax import lax
from jax.experimental import pallas as pl
from jax.experimental.pallas import tpu as pltpu
from jax.sharding import PartitionSpec as P

ITERS = 4
LANES = 128
SUB = 8
WIDE = 256
VEL = 6
PROPS = 4
MAIL = 7
relax = 0.1
MESH = pl.DeviceIdType.MESH
KEEP_BYTES = 24 * 1024 * 1024
HOT = jnp.float8_e4m3fn
PAIRED = 2


def cross_rows(left, right):
    return [
        left[1] * right[2] - left[2] * right[1],
        left[2] * right[0] - left[0] * right[2],
        left[0] * right[1] - left[1] * right[0],
    ]


def remote(source, target, send_sem, recv_sem, where):
    return pltpu.make_async_remote_copy(
        src_ref=source,
        dst_ref=target,
        send_sem=send_sem,
        recv_sem=recv_sem,
        device_id=where,
        device_id_type=MESH,
    )


def flip(sub, stage):
    step = 2**stage
    return sub + step - 2 * step * ((sub // step) % 2)


def spread(row, height):
    return jnp.broadcast_to(row, (height, LANES))


def kernel(
    groups, subs, height, blocks, span, keep, relaxed,
    vel_any, prop_any, first_any, second_any, raw_any, target_any, live_any, imp_any,
    vel_out, imp_out,
    vel_ref, prop_ref, first_ref, second_ref, raw_ref, target_ref, live_ref, imp_ref,
    geo_ref, table, wide_parts, parts, onehot, low_s, chunk_s, jac, gain, imp, coef, rowbuf,
    acc, mail_out, mail_in, mass_out, mass_in, talk_out, talk_in, red_out, red_in,
    s_load, s_mail, r_mail, s_mass, r_mass, s_talk, r_talk, s_red, r_red,
):
    owner, sub = lax.axis_index("owner"), lax.axis_index("sub")
    stages = subs.bit_length() - 1
    rows = VEL * height
    every = (VEL + PROPS) * height
    owned = height * WIDE
    full = (groups - 1) // PAIRED
    head = groups - PAIRED * full
    mirrored = groups & (groups - 1) == 0

    def partner(k):
        if not mirrored:
            return lax.rem(owner + k, groups)
        q = owner
        for bit in range(groups.bit_length() - 1):
            step = 2**bit
            chosen = lax.rem(lax.div(k, step), 2) if not isinstance(k, int) else k // step % 2
            q = q + chosen * (step - 2 * step * lax.rem(lax.div(owner, step), 2))
        return q

    def there(k):
        return k if mirrored else lax.rem(groups - k, groups)

    barrier = pltpu.get_barrier_semaphore()

    def signal(k, carry):
        pl.semaphore_signal(
            barrier, inc=1, device_id=(partner(k), sub), device_id_type=MESH
        )
        return carry

    lax.fori_loop(1, groups, signal, 0)
    for stage in range(stages):
        pl.semaphore_signal(
            barrier, inc=1, device_id=(owner, flip(sub, stage)), device_id_type=MESH
        )

    loads = [
        pltpu.make_async_copy(source, target, s_load.at[n])
        for n, (source, target) in enumerate(
            [
                (raw_any, raw_ref),
                (live_any, live_ref),
                (second_any, second_ref),
                (first_any, first_ref),
                (vel_any, vel_ref),
                (prop_any, prop_ref),
                (target_any, target_ref),
                (imp_any, imp_ref),
            ]
        )
    ]
    for load in loads:
        load.start()

    def link(source, target, send_sem, recv_sem):
        def outgoing(k, *at):
            return remote(
                source.at[(*at, k)], target.at[(*at, there(k))], send_sem.at[(*at, k)],
                recv_sem.at[(*at, there(k))], (partner(k), sub),
            )

        def incoming(k, *at):
            return remote(
                source.at[(*at, k)], target.at[(*at, k)], send_sem.at[(*at, k)],
                recv_sem.at[(*at, k)], (partner(k), sub),
            )

        return outgoing, incoming

    mail, mail_here = link(mail_out, mail_in, s_mail, r_mail)
    mass, mass_here = link(mass_out, mass_in, s_mass, r_mass)
    talk, talk_here = link(talk_out, talk_in, s_talk, r_talk)

    def part(b):
        return pl.ds(b * SUB, SUB)

    def over_blocks(body):
        if blocks == 1:
            body(0)
        else:
            def run(b, carry):
                body(b)
                return carry

            lax.fori_loop(0, blocks, run, 0)

    def far_first(body):
        def run(j, carry):
            body([groups - 1 - PAIRED * j - n for n in range(PAIRED)])
            return carry

        lax.fori_loop(0, full, run, 0)
        body(list(range(head - 1, -1, -1)))

    def near_first(body):
        def run(j, carry):
            body([head + PAIRED * j + n for n in range(PAIRED)])
            return carry

        body(list(range(head)))
        lax.fori_loop(0, full, run, 0)

    def here(k):
        return isinstance(k, int) and k == 0

    def live_of(q, b):
        lane = lax.broadcasted_iota(jnp.int32, (SUB, LANES), 1)
        line = lax.broadcasted_iota(jnp.int32, (SUB, LANES), 0)
        bound = jnp.zeros((SUB, LANES), jnp.int32)
        for i in range(SUB):
            row = (q * blocks + b) * SUB + i
            left = live_ref[row // span] - (row % span) * LANES
            bound = jnp.where(line == i, left, bound)
        return lane < bound

    def local(index):
        return index - lax.div(index, jnp.full_like(index, owned)) * owned

    def write_mail(k, carry):
        q = partner(k)

        def block(b):
            for r in range(9):
                for i in range(SUB):
                    start = pl.multiple_of(((q * blocks + b) * SUB + i) * LANES, LANES)
                    geo_ref[r, k, pl.ds(b * SUB + i, 1), :] = raw_ref[
                        pl.ds(r, 1), pl.ds(start, LANES)
                    ]
            normal = [geo_ref[r, k, part(b)] for r in range(3)]
            cross = cross_rows([geo_ref[6 + r, k, part(b)] for r in range(3)], normal)
            live = live_of(q, b)
            for r, value in enumerate(normal + cross):
                mail_out[k, r, part(b)] = jnp.where(live, -value, 0.0)
            mail_out[k, VEL, part(b)] = local(second_ref[q, part(b)]).astype(jnp.float32)

        over_blocks(block)
        return carry

    for load in loads[:3]:
        load.wait()
    lax.fori_loop(0, groups, write_mail, 0)
    for load in loads[3:]:
        load.wait()

    for r in range(VEL):
        for c in range(height):
            table[pl.ds(r * height + c, 1), :] = vel_ref[pl.ds(r, 1), pl.ds(c * WIDE, WIDE)]
    for r in range(PROPS):
        for c in range(height):
            rowbuf[pl.ds(r * height + c, 1), :] = prop_ref[pl.ds(r, 1), pl.ds(c * WIDE, WIDE)]
    whole = jnp.concatenate([table[...], rowbuf[...]], axis=0)
    whole_high = whole.astype(jnp.bfloat16)
    wide_parts[pl.ds(0, every), :] = whole_high
    wide_parts[pl.ds(every, every), :] = (whole - whole_high.astype(jnp.float32)).astype(
        jnp.bfloat16
    )

    def hot(low, i):
        tall = lax.broadcasted_iota(jnp.int32, (WIDE, LANES), 0)
        return jnp.where(tall == spread(low[i : i + 1], WIDE), 1.0, 0.0).astype(HOT)

    def hot_tile(side, k, b):
        if keep:
            return onehot[side, k, b]
        low = low_s[side, k, part(b)]
        return jnp.concatenate([hot(low, i) for i in range(SUB)], axis=1)

    def hits(chunk):
        tall = lax.broadcasted_iota(jnp.int32, (height, LANES), 0)
        return [tall == spread(chunk[i : i + 1], height) for i in range(SUB)]

    def picked(values, tile):
        half = values.shape[0] // 2
        out = lax.dot_general(
            values[...], tile, (((1,), (0,)), ((), ())), preferred_element_type=jnp.float32
        )
        return out[:half] + out[half:]

    def lookup(got, masks, lines):
        found = []
        for i in range(SUB):
            total = None
            for r, line in lines:
                piece = got[r * height : (r + 1) * height, i * LANES : (i + 1) * LANES]
                if line is not None:
                    piece = piece * spread(line(i), height)
                total = piece if total is None else total + piece
            found.append(jnp.sum(jnp.where(masks[i], total, 0.0), axis=0, keepdims=True))
        return jnp.concatenate(found, axis=0)

    def prepare(side, k, b, index, values, aim):
        low = lax.rem(index, jnp.full_like(index, WIDE))
        chunk = lax.div(index, jnp.full_like(index, WIDE))
        low_s[side, k, part(b)] = low
        chunk_s[side, k, part(b)] = chunk
        pieces = [hot(low, i) for i in range(SUB)]
        if keep:
            for i in range(SUB):
                onehot[side, k, b, :, pl.ds(i * LANES, LANES)] = pieces[i]
        got = picked(wide_parts, jnp.concatenate(pieces, axis=1))
        masks = hits(chunk)
        prop = [lookup(got, masks, [(VEL + r, None)]) for r in range(PROPS)]
        speed = lookup(
            got, masks, [(r, lambda i, r=r: values[r][i : i + 1]) for r in range(VEL)]
        )
        total = prop[0]
        for r in range(VEL):
            jac[side, k, r, part(b)] = values[r]
            gain[side, k, r, part(b)] = prop[max(0, r - 2)] * values[r]
        for r in range(3):
            total += values[3 + r] * values[3 + r] * prop[1 + r]
        mass_out[k, side, part(b)] = total
        talk_out[0, k, side, part(b)] = aim - speed

    def prepare_first(ks):
        def block(b):
            for k in ks:
                q = partner(k)
                normal = [geo_ref[r, k, part(b)] for r in range(3)]
                cross = cross_rows([geo_ref[3 + r, k, part(b)] for r in range(3)], normal)
                index = local(first_ref[q, part(b)])
                prepare(0, k, b, index, normal + cross, target_ref[q, part(b)])
                start = imp_ref[q, part(b)]
                imp[0, k, part(b)] = start
                mass_out[k, 2, part(b)] = start

        over_blocks(block)

    def prepare_second(ks):
        for k in ks:
            if not here(k):
                mail_here(k).wait_recv()

        def block(b):
            for k in ks:
                source = mail_out if here(k) else mail_in
                values = [source[k, r, part(b)] for r in range(VEL)]
                index = source[k, VEL, part(b)].astype(jnp.int32)
                prepare(1, k, b, index, values, 0.0)

        over_blocks(block)
        for k in ks:
            if not here(k):
                mass(k).start()
                talk(k, 0).start()

    def post(j, carry):
        mail(groups - j).start()
        return carry

    far_first(prepare_first)
    pl.semaphore_wait(barrier, groups - 1 + stages)
    lax.fori_loop(1, groups, post, 0)
    far_first(prepare_second)

    def speak(t):
        def some(ks):
            def block(b):
                for k, side in [(k, side) for k in ks for side in range(2)]:
                    got = picked(parts, hot_tile(side, k, b))
                    masks = hits(chunk_s[side, k, part(b)])
                    lines = [
                        (r, lambda i, r=r: jac[side, k, r, pl.ds(b * SUB + i, 1)])
                        for r in range(VEL)
                    ]
                    aim = target_ref[partner(k), part(b)] if side == 0 else 0.0
                    talk_out[t, k, side, part(b)] = aim - lookup(got, masks, lines)

            over_blocks(block)
            for k in ks:
                if not here(k):
                    talk(k, t).start()

        far_first(some)

    def place(deltas, side, k, b):
        coarse = [d.astype(jnp.bfloat16).astype(jnp.float32) for d in deltas]
        fine = [d - c for d, c in zip(deltas, coarse)]
        masks = hits(chunk_s[side, k, part(b)])
        left = []
        for i in range(SUB):
            lines = [
                jnp.where(masks[i], spread(x[i : i + 1], height), 0.0) for x in coarse + fine
            ]
            left.append(jnp.concatenate(lines, axis=0).astype(jnp.bfloat16))
        out = lax.dot_general(
            jnp.concatenate(left, axis=1),
            hot_tile(side, k, b),
            (((1,), (1,)), ((), ())),
            preferred_element_type=jnp.float32,
        )
        return out[:rows] + out[rows:]

    def settle(k, b):
        peer_ref = mass_out if here(k) else mass_in
        for side in range(2):
            value = relaxed / (mass_out[k, side, part(b)] + peer_ref[k, 1 - side, part(b)])
            if side == 0:
                value = jnp.where(live_of(partner(k), b), value, 0.0)
            coef[side, k, part(b)] = value
        imp[1, k, part(b)] = peer_ref[k, 2, part(b)]

    def act(t, first):
        acc[...] = jnp.zeros_like(acc)

        def some(ks):
            for k in ks:
                if not here(k):
                    talk_here(k, t).wait_recv()
                    if first:
                        mass_here(k).wait_recv()

            def block(b):
                moved = []
                for k in ks:
                    if first:
                        settle(k, b)
                    peer_ref = talk_out if here(k) else talk_in
                    for side in range(2):
                        push = (
                            talk_out[t, k, side, part(b)] + peer_ref[t, k, 1 - side, part(b)]
                        )
                        before = imp[side, k, part(b)]
                        fresh = jnp.maximum(before + push * coef[side, k, part(b)], 0.0)
                        imp[side, k, part(b)] = fresh
                        applied = fresh - before
                        deltas = [applied * gain[side, k, r, part(b)] for r in range(VEL)]
                        moved.append(place(deltas, side, k, b))
                acc[...] += functools.reduce(jnp.add, moved)

            over_blocks(block)

        near_first(some)

    def reduce(t, stage):
        return remote(
            red_out.at[t, stage], red_in.at[t, stage], s_red.at[t, stage],
            r_red.at[t, stage], (owner, flip(sub, stage)),
        )

    def advance(t):
        total = acc[...]
        for stage in range(stages):
            red_out[t, stage] = total
            reduce(t, stage).start()
            reduce(t, stage).wait_recv()
            total = total + red_in[t, stage]
        value = table[...] + total
        table[...] = value
        high = value.astype(jnp.bfloat16)
        parts[pl.ds(0, rows), :] = high
        parts[pl.ds(rows, rows), :] = (value - high.astype(jnp.float32)).astype(jnp.bfloat16)

    act(0, True)
    advance(0)

    def iteration(t, carry):
        speak(t)
        act(t, False)
        advance(t)
        return carry

    lax.fori_loop(1, ITERS, iteration, 0)

    for r in range(VEL):
        for c in range(height):
            vel_out[pl.ds(r, 1), pl.ds(c * WIDE, WIDE)] = table[pl.ds(r * height + c, 1), :]

    def finish(k, carry):
        imp_out[partner(k)] = imp[0, k]
        return carry

    lax.fori_loop(0, groups, finish, 0)

    def sent(k, carry):
        mail(k).wait_send()
        mass(k).wait_send()
        for t in range(ITERS):
            talk(k, t).wait_send()
        return carry

    lax.fori_loop(1, groups, sent, 0)
    for t in range(ITERS):
        for stage in range(stages):
            reduce(t, stage).wait_send()


def on_device(
    groups, subs, velocity, properties, first_body, second_body, geometry, target_speed,
    warm_impulse, live_pairs
):
    owned = velocity.shape[1]
    height = owned // WIDE
    count = first_body.shape[0]
    rows = count // (groups * LANES)
    blocks = rows // SUB
    tiles = (groups, rows, LANES)
    stages = subs.bit_length() - 1
    keep = 2 * count * WIDE <= KEEP_BYTES
    kept = (2, groups, blocks, WIDE, SUB * LANES) if keep else (1, 1, 1, 32, LANES)
    span = count // live_pairs.shape[0] // LANES

    f32 = jnp.float32
    pair = (2, groups, rows, LANES)
    operands = (
        velocity,
        properties,
        first_body.reshape(tiles),
        second_body.reshape(tiles),
        geometry,
        target_speed.reshape(tiles),
        live_pairs,
        warm_impulse.reshape(tiles),
    )
    held = [pltpu.VMEM(x.shape, x.dtype) for x in operands]
    held[6] = pltpu.SMEM(live_pairs.shape, live_pairs.dtype)
    speeds, impulse = pl.pallas_call(
        functools.partial(kernel, groups, subs, height, blocks, span, keep, relax),
        name="contacts",
        out_shape=(
            jax.ShapeDtypeStruct((VEL, owned), f32),
            jax.ShapeDtypeStruct(tiles, f32),
        ),
        in_specs=[pl.BlockSpec(memory_space=pl.ANY)] * 8,
        out_specs=(pl.BlockSpec(memory_space=pltpu.VMEM),) * 2,
        scratch_shapes=held
        + [
            pltpu.VMEM((geometry.shape[0],) + tiles, f32),
            pltpu.VMEM((VEL * height, WIDE), f32),
            pltpu.VMEM((2 * (VEL + PROPS) * height, WIDE), jnp.bfloat16),
            pltpu.VMEM((2 * VEL * height, WIDE), jnp.bfloat16),
            pltpu.VMEM(kept, HOT),
            pltpu.VMEM(pair, jnp.int32),
            pltpu.VMEM(pair, jnp.int32),
            pltpu.VMEM((2, groups, VEL, rows, LANES), f32),
            pltpu.VMEM((2, groups, VEL, rows, LANES), f32),
            pltpu.VMEM(pair, f32),
            pltpu.VMEM(pair, f32),
            pltpu.VMEM((PROPS * height, WIDE), f32),
            pltpu.VMEM((VEL * height, WIDE), f32),
            pltpu.VMEM((groups, MAIL, rows, LANES), f32),
            pltpu.VMEM((groups, MAIL, rows, LANES), f32),
            pltpu.VMEM((groups, 3, rows, LANES), f32),
            pltpu.VMEM((groups, 3, rows, LANES), f32),
            pltpu.VMEM((ITERS, groups, 2, rows, LANES), f32),
            pltpu.VMEM((ITERS, groups, 2, rows, LANES), f32),
            pltpu.VMEM((ITERS, stages, VEL * height, WIDE), f32),
            pltpu.VMEM((ITERS, stages, VEL * height, WIDE), f32),
            pltpu.SemaphoreType.DMA((len(operands),)),
        ]
        + [pltpu.SemaphoreType.DMA((groups,))] * 4
        + [pltpu.SemaphoreType.DMA((ITERS, groups))] * 2
        + [pltpu.SemaphoreType.DMA((ITERS, stages))] * 2,
        compiler_params=pltpu.CompilerParams(collective_id=0, has_side_effects=True),
    )(*operands)
    return (speeds, impulse.reshape(count))


def solution(mesh):
    groups, subs = mesh.shape["owner"], mesh.shape["sub"]
    return jax.shard_map(
        functools.partial(on_device, groups, subs),
        mesh=mesh,
        in_specs=(
            P(None, "owner"),
            P(None, "owner"),
            P(("owner", "sub")),
            P(("owner", "sub")),
            P(None, ("owner", "sub")),
            P(("owner", "sub")),
            P(("owner", "sub")),
            P(("owner", "sub")),
        ),
        out_specs=(P(None, "owner"), P(("owner", "sub"))),
        check_vma=False,
    )
```

```python
import functools

import jax
import jax.numpy as jnp
from jax import lax
from jax.experimental import pallas as pl
from jax.experimental.pallas import tpu as pltpu
from jax.sharding import PartitionSpec as P

ITERS = 4
LANES = 128
SUB = 8
WIDE = 256
VEL = 6
PROPS = 4
MAIL = 7
relax = 0.1
MESH = pl.DeviceIdType.MESH
KEEP_BYTES = 24 * 1024 * 1024
HOT = jnp.float8_e4m3fn
PAIRED = 2


def cross_rows(left, right):
    return [
        left[1] * right[2] - left[2] * right[1],
        left[2] * right[0] - left[0] * right[2],
        left[0] * right[1] - left[1] * right[0],
    ]


def remote(source, target, send_sem, recv_sem, where):
    return pltpu.make_async_remote_copy(
        src_ref=source,
        dst_ref=target,
        send_sem=send_sem,
        recv_sem=recv_sem,
        device_id=where,
        device_id_type=MESH,
    )


def flip(sub, stage):
    step = 2**stage
    return sub + step - 2 * step * ((sub // step) % 2)


def across(sub, distance):
    for stage in range(distance.bit_length()):
        if distance >> stage & 1:
            sub = flip(sub, stage)
    return sub


def spread(row, height):
    return jnp.broadcast_to(row, (height, LANES))


def kernel(
    groups, subs, height, blocks, span, keep, relaxed,
    vel_any, prop_any, first_any, second_any, raw_any, target_any, live_any, imp_any,
    vel_out, imp_out,
    vel_ref, prop_ref, first_ref, second_ref, raw_ref, target_ref, live_ref, imp_ref,
    geo_ref, table, wide_parts, parts, onehot, low_s, chunk_s, jac, gain, imp, coef, rowbuf,
    acc, mail_out, mail_in, mass_out, mass_in, talk_out, talk_in, red_out, red_in,
    s_load, s_mail, r_mail, s_mass, r_mass, s_talk, r_talk, s_red, r_red,
):
    owner, sub = lax.axis_index("owner"), lax.axis_index("sub")
    rows = VEL * height
    every = (VEL + PROPS) * height
    owned = height * WIDE
    full = (groups - 1) // PAIRED
    head = groups - PAIRED * full
    mirrored = groups & (groups - 1) == 0

    def partner(k):
        if not mirrored:
            return lax.rem(owner + k, groups)
        q = owner
        for bit in range(groups.bit_length() - 1):
            step = 2**bit
            chosen = lax.rem(lax.div(k, step), 2) if not isinstance(k, int) else k // step % 2
            q = q + chosen * (step - 2 * step * lax.rem(lax.div(owner, step), 2))
        return q

    def there(k):
        return k if mirrored else lax.rem(groups - k, groups)

    barrier = pltpu.get_barrier_semaphore()

    def signal(k, carry):
        pl.semaphore_signal(
            barrier, inc=1, device_id=(partner(k), sub), device_id_type=MESH
        )
        return carry

    lax.fori_loop(1, groups, signal, 0)
    for j in range(1, subs):
        pl.semaphore_signal(
            barrier, inc=1, device_id=(owner, across(sub, j)), device_id_type=MESH
        )

    loads = [
        pltpu.make_async_copy(source, target, s_load.at[n])
        for n, (source, target) in enumerate(
            [
                (raw_any, raw_ref),
                (live_any, live_ref),
                (second_any, second_ref),
                (first_any, first_ref),
                (vel_any, vel_ref),
                (prop_any, prop_ref),
                (target_any, target_ref),
                (imp_any, imp_ref),
            ]
        )
    ]
    for load in loads:
        load.start()

    def link(source, target, send_sem, recv_sem):
        def outgoing(k, *at):
            return remote(
                source.at[(*at, k)], target.at[(*at, there(k))], send_sem.at[(*at, k)],
                recv_sem.at[(*at, there(k))], (partner(k), sub),
            )

        def incoming(k, *at):
            return remote(
                source.at[(*at, k)], target.at[(*at, k)], send_sem.at[(*at, k)],
                recv_sem.at[(*at, k)], (partner(k), sub),
            )

        return outgoing, incoming

    mail, mail_here = link(mail_out, mail_in, s_mail, r_mail)
    mass, mass_here = link(mass_out, mass_in, s_mass, r_mass)
    talk, talk_here = link(talk_out, talk_in, s_talk, r_talk)

    def part(b):
        return pl.ds(b * SUB, SUB)

    def over_blocks(body):
        if blocks == 1:
            body(0)
        else:
            def run(b, carry):
                body(b)
                return carry

            lax.fori_loop(0, blocks, run, 0)

    def far_first(body):
        def run(j, carry):
            body([groups - 1 - PAIRED * j - n for n in range(PAIRED)])
            return carry

        lax.fori_loop(0, full, run, 0)
        body(list(range(head - 1, -1, -1)))

    def near_first(body):
        def run(j, carry):
            body([head + PAIRED * j + n for n in range(PAIRED)])
            return carry

        body(list(range(head)))
        lax.fori_loop(0, full, run, 0)

    def here(k):
        return isinstance(k, int) and k == 0

    def live_of(q, b):
        lane = lax.broadcasted_iota(jnp.int32, (SUB, LANES), 1)
        line = lax.broadcasted_iota(jnp.int32, (SUB, LANES), 0)
        bound = jnp.zeros((SUB, LANES), jnp.int32)
        for i in range(SUB):
            row = (q * blocks + b) * SUB + i
            left = live_ref[row // span] - (row % span) * LANES
            bound = jnp.where(line == i, left, bound)
        return lane < bound

    def local(index):
        return index - lax.div(index, jnp.full_like(index, owned)) * owned

    def write_mail(k, carry):
        q = partner(k)

        def block(b):
            for r in range(9):
                for i in range(SUB):
                    start = pl.multiple_of(((q * blocks + b) * SUB + i) * LANES, LANES)
                    geo_ref[r, k, pl.ds(b * SUB + i, 1), :] = raw_ref[
                        pl.ds(r, 1), pl.ds(start, LANES)
                    ]
            normal = [geo_ref[r, k, part(b)] for r in range(3)]
            cross = cross_rows([geo_ref[6 + r, k, part(b)] for r in range(3)], normal)
            live = live_of(q, b)
            for r, value in enumerate(normal + cross):
                mail_out[k, r, part(b)] = jnp.where(live, -value, 0.0)
            mail_out[k, VEL, part(b)] = local(second_ref[q, part(b)]).astype(jnp.float32)

        over_blocks(block)
        return carry

    for load in loads[:3]:
        load.wait()
    lax.fori_loop(0, groups, write_mail, 0)
    for load in loads[3:]:
        load.wait()

    for r in range(VEL):
        for c in range(height):
            table[pl.ds(r * height + c, 1), :] = vel_ref[pl.ds(r, 1), pl.ds(c * WIDE, WIDE)]
    for r in range(PROPS):
        for c in range(height):
            rowbuf[pl.ds(r * height + c, 1), :] = prop_ref[pl.ds(r, 1), pl.ds(c * WIDE, WIDE)]
    whole = jnp.concatenate([table[...], rowbuf[...]], axis=0)
    whole_high = whole.astype(jnp.bfloat16)
    wide_parts[pl.ds(0, every), :] = whole_high
    wide_parts[pl.ds(every, every), :] = (whole - whole_high.astype(jnp.float32)).astype(
        jnp.bfloat16
    )

    def hot(low, i):
        tall = lax.broadcasted_iota(jnp.int32, (WIDE, LANES), 0)
        return jnp.where(tall == spread(low[i : i + 1], WIDE), 1.0, 0.0).astype(HOT)

    def hot_tile(side, k, b):
        if keep:
            return onehot[side, k, b]
        low = low_s[side, k, part(b)]
        return jnp.concatenate([hot(low, i) for i in range(SUB)], axis=1)

    def hits(chunk):
        tall = lax.broadcasted_iota(jnp.int32, (height, LANES), 0)
        return [tall == spread(chunk[i : i + 1], height) for i in range(SUB)]

    def picked(values, tile):
        half = values.shape[0] // 2
        out = lax.dot_general(
            values[...], tile, (((1,), (0,)), ((), ())), preferred_element_type=jnp.float32
        )
        return out[:half] + out[half:]

    def lookup(got, masks, lines):
        found = []
        for i in range(SUB):
            total = None
            for r, line in lines:
                piece = got[r * height : (r + 1) * height, i * LANES : (i + 1) * LANES]
                if line is not None:
                    piece = piece * spread(line(i), height)
                total = piece if total is None else total + piece
            found.append(jnp.sum(jnp.where(masks[i], total, 0.0), axis=0, keepdims=True))
        return jnp.concatenate(found, axis=0)

    def prepare(side, k, b, index, values, aim):
        low = lax.rem(index, jnp.full_like(index, WIDE))
        chunk = lax.div(index, jnp.full_like(index, WIDE))
        low_s[side, k, part(b)] = low
        chunk_s[side, k, part(b)] = chunk
        pieces = [hot(low, i) for i in range(SUB)]
        if keep:
            for i in range(SUB):
                onehot[side, k, b, :, pl.ds(i * LANES, LANES)] = pieces[i]
        got = picked(wide_parts, jnp.concatenate(pieces, axis=1))
        masks = hits(chunk)
        prop = [lookup(got, masks, [(VEL + r, None)]) for r in range(PROPS)]
        speed = lookup(
            got, masks, [(r, lambda i, r=r: values[r][i : i + 1]) for r in range(VEL)]
        )
        total = prop[0]
        for r in range(VEL):
            jac[side, k, r, part(b)] = values[r]
            gain[side, k, r, part(b)] = prop[max(0, r - 2)] * values[r]
        for r in range(3):
            total += values[3 + r] * values[3 + r] * prop[1 + r]
        mass_out[k, side, part(b)] = total
        talk_out[0, k, side, part(b)] = aim - speed

    def prepare_first(ks):
        def block(b):
            for k in ks:
                q = partner(k)
                normal = [geo_ref[r, k, part(b)] for r in range(3)]
                cross = cross_rows([geo_ref[3 + r, k, part(b)] for r in range(3)], normal)
                index = local(first_ref[q, part(b)])
                prepare(0, k, b, index, normal + cross, target_ref[q, part(b)])
                start = imp_ref[q, part(b)]
                imp[0, k, part(b)] = start
                mass_out[k, 2, part(b)] = start

        over_blocks(block)

    def prepare_second(ks):
        for k in ks:
            if not here(k):
                mail_here(k).wait_recv()

        def block(b):
            for k in ks:
                source = mail_out if here(k) else mail_in
                values = [source[k, r, part(b)] for r in range(VEL)]
                index = source[k, VEL, part(b)].astype(jnp.int32)
                prepare(1, k, b, index, values, 0.0)

        over_blocks(block)
        for k in ks:
            if not here(k):
                mass(k).start()
                talk(k, 0).start()

    def post(j, carry):
        mail(j).start()
        return carry

    far_first(prepare_first)
    pl.semaphore_wait(barrier, groups + subs - 2)
    lax.fori_loop(1, groups, post, 0)
    near_first(prepare_second)

    def speak(t):
        def some(ks):
            def block(b):
                for k, side in [(k, side) for k in ks for side in range(2)]:
                    got = picked(parts, hot_tile(side, k, b))
                    masks = hits(chunk_s[side, k, part(b)])
                    lines = [
                        (r, lambda i, r=r: jac[side, k, r, pl.ds(b * SUB + i, 1)])
                        for r in range(VEL)
                    ]
                    aim = target_ref[partner(k), part(b)] if side == 0 else 0.0
                    talk_out[t, k, side, part(b)] = aim - lookup(got, masks, lines)

            over_blocks(block)
            for k in ks:
                if not here(k):
                    talk(k, t).start()

        far_first(some)

    def place(deltas, side, k, b):
        coarse = [d.astype(jnp.bfloat16).astype(jnp.float32) for d in deltas]
        fine = [d - c for d, c in zip(deltas, coarse)]
        masks = hits(chunk_s[side, k, part(b)])
        left = []
        for i in range(SUB):
            lines = [
                jnp.where(masks[i], spread(x[i : i + 1], height), 0.0) for x in coarse + fine
            ]
            left.append(jnp.concatenate(lines, axis=0).astype(jnp.bfloat16))
        out = lax.dot_general(
            jnp.concatenate(left, axis=1),
            hot_tile(side, k, b),
            (((1,), (1,)), ((), ())),
            preferred_element_type=jnp.float32,
        )
        return out[:rows] + out[rows:]

    def settle(k, b):
        peer_ref = mass_out if here(k) else mass_in
        for side in range(2):
            value = relaxed / (mass_out[k, side, part(b)] + peer_ref[k, 1 - side, part(b)])
            if side == 0:
                value = jnp.where(live_of(partner(k), b), value, 0.0)
            coef[side, k, part(b)] = value
        imp[1, k, part(b)] = peer_ref[k, 2, part(b)]

    def act(t, first):
        acc[...] = jnp.zeros_like(acc)

        def some(ks):
            for k in ks:
                if not here(k):
                    talk_here(k, t).wait_recv()
                    if first:
                        mass_here(k).wait_recv()

            def block(b):
                moved = []
                for k in ks:
                    if first:
                        settle(k, b)
                    peer_ref = talk_out if here(k) else talk_in
                    for side in range(2):
                        push = (
                            talk_out[t, k, side, part(b)] + peer_ref[t, k, 1 - side, part(b)]
                        )
                        before = imp[side, k, part(b)]
                        fresh = jnp.maximum(before + push * coef[side, k, part(b)], 0.0)
                        imp[side, k, part(b)] = fresh
                        applied = fresh - before
                        deltas = [applied * gain[side, k, r, part(b)] for r in range(VEL)]
                        moved.append(place(deltas, side, k, b))
                acc[...] += functools.reduce(jnp.add, moved)

            over_blocks(block)

        near_first(some)

    def reduce(t, j):
        return remote(
            red_out.at[t], red_in.at[t, j], s_red.at[t, j], r_red.at[t, j],
            (owner, across(sub, j)),
        )

    def advance(t):
        red_out[t] = acc[...]
        for j in range(1, subs):
            reduce(t, j).start()
        terms = [acc[...]]
        for j in range(1, subs):
            reduce(t, j).wait_recv()
            terms.append(red_in[t, j])
        while len(terms) > 1:
            terms = [a + b for a, b in zip(terms[::2], terms[1::2])]
        value = table[...] + terms[0]
        table[...] = value
        high = value.astype(jnp.bfloat16)
        parts[pl.ds(0, rows), :] = high
        parts[pl.ds(rows, rows), :] = (value - high.astype(jnp.float32)).astype(jnp.bfloat16)

    act(0, True)
    advance(0)

    def iteration(t, carry):
        speak(t)
        act(t, False)
        advance(t)
        return carry

    lax.fori_loop(1, ITERS, iteration, 0)

    for r in range(VEL):
        for c in range(height):
            vel_out[pl.ds(r, 1), pl.ds(c * WIDE, WIDE)] = table[pl.ds(r * height + c, 1), :]

    def finish(k, carry):
        imp_out[partner(k)] = imp[0, k]
        return carry

    lax.fori_loop(0, groups, finish, 0)

    def sent(k, carry):
        mail(k).wait_send()
        mass(k).wait_send()
        for t in range(ITERS):
            talk(k, t).wait_send()
        return carry

    lax.fori_loop(1, groups, sent, 0)
    for t in range(ITERS):
        for j in range(1, subs):
            reduce(t, j).wait_send()


def on_device(
    groups, subs, velocity, properties, first_body, second_body, geometry, target_speed,
    warm_impulse, live_pairs
):
    owned = velocity.shape[1]
    height = owned // WIDE
    count = first_body.shape[0]
    rows = count // (groups * LANES)
    blocks = rows // SUB
    tiles = (groups, rows, LANES)
    keep = 2 * count * WIDE <= KEEP_BYTES
    kept = (2, groups, blocks, WIDE, SUB * LANES) if keep else (1, 1, 1, 32, LANES)
    span = count // live_pairs.shape[0] // LANES

    f32 = jnp.float32
    pair = (2, groups, rows, LANES)
    operands = (
        velocity,
        properties,
        first_body.reshape(tiles),
        second_body.reshape(tiles),
        geometry,
        target_speed.reshape(tiles),
        live_pairs,
        warm_impulse.reshape(tiles),
    )
    held = [pltpu.VMEM(x.shape, x.dtype) for x in operands]
    held[6] = pltpu.SMEM(live_pairs.shape, live_pairs.dtype)
    speeds, impulse = pl.pallas_call(
        functools.partial(kernel, groups, subs, height, blocks, span, keep, relax),
        name="contacts",
        out_shape=(
            pltpu.VMEM((VEL, owned), f32),
            pltpu.VMEM(tiles, f32),
        ),
        in_specs=[pl.BlockSpec(memory_space=pl.ANY)] * 8,
        out_specs=(pl.BlockSpec(memory_space=pltpu.VMEM),) * 2,
        scratch_shapes=held
        + [
            pltpu.VMEM((geometry.shape[0],) + tiles, f32),
            pltpu.VMEM((VEL * height, WIDE), f32),
            pltpu.VMEM((2 * (VEL + PROPS) * height, WIDE), jnp.bfloat16),
            pltpu.VMEM((2 * VEL * height, WIDE), jnp.bfloat16),
            pltpu.VMEM(kept, HOT),
            pltpu.VMEM(pair, jnp.int32),
            pltpu.VMEM(pair, jnp.int32),
            pltpu.VMEM((2, groups, VEL, rows, LANES), f32),
            pltpu.VMEM((2, groups, VEL, rows, LANES), f32),
            pltpu.VMEM(pair, f32),
            pltpu.VMEM(pair, f32),
            pltpu.VMEM((PROPS * height, WIDE), f32),
            pltpu.VMEM((VEL * height, WIDE), f32),
            pltpu.VMEM((groups, MAIL, rows, LANES), f32),
            pltpu.VMEM((groups, MAIL, rows, LANES), f32),
            pltpu.VMEM((groups, 3, rows, LANES), f32),
            pltpu.VMEM((groups, 3, rows, LANES), f32),
            pltpu.VMEM((ITERS, groups, 2, rows, LANES), f32),
            pltpu.VMEM((ITERS, groups, 2, rows, LANES), f32),
            pltpu.VMEM((ITERS, VEL * height, WIDE), f32),
            pltpu.VMEM((ITERS, subs, VEL * height, WIDE), f32),
            pltpu.SemaphoreType.DMA((len(operands),)),
        ]
        + [pltpu.SemaphoreType.DMA((groups,))] * 4
        + [pltpu.SemaphoreType.DMA((ITERS, groups))] * 2
        + [pltpu.SemaphoreType.DMA((ITERS, subs))] * 2,
        compiler_params=pltpu.CompilerParams(collective_id=0, has_side_effects=True),
    )(*operands)
    return (speeds, impulse.reshape(count))


def solution(mesh):
    groups, subs = mesh.shape["owner"], mesh.shape["sub"]
    return jax.shard_map(
        functools.partial(on_device, groups, subs),
        mesh=mesh,
        in_specs=(
            P(None, "owner"),
            P(None, "owner"),
            P(("owner", "sub")),
            P(("owner", "sub")),
            P(None, ("owner", "sub")),
            P(("owner", "sub")),
            P(("owner", "sub")),
            P(("owner", "sub")),
        ),
        out_specs=(P(None, "owner"), P(("owner", "sub"))),
        check_vma=False,
    )
```

```python
import functools

import jax
import jax.numpy as jnp
from jax import lax
from jax.experimental import pallas as pl
from jax.experimental.pallas import tpu as pltpu
from jax.sharding import PartitionSpec as P

ITERS = 4
LANES = 128
SUB = 8
WIDE = 256
VEL = 6
PROPS = 4
MAIL = 7
relax = 0.1
MESH = pl.DeviceIdType.MESH
KEEP_BYTES = 24 * 1024 * 1024
HOT = jnp.float8_e4m3fn
PAIRED = 2


def cross_rows(left, right):
    return [
        left[1] * right[2] - left[2] * right[1],
        left[2] * right[0] - left[0] * right[2],
        left[0] * right[1] - left[1] * right[0],
    ]


def remote(source, target, send_sem, recv_sem, where):
    return pltpu.make_async_remote_copy(
        src_ref=source,
        dst_ref=target,
        send_sem=send_sem,
        recv_sem=recv_sem,
        device_id=where,
        device_id_type=MESH,
    )


def flip(sub, stage):
    step = 2**stage
    return sub + step - 2 * step * ((sub // step) % 2)


def across(sub, distance):
    for stage in range(distance.bit_length()):
        if distance >> stage & 1:
            sub = flip(sub, stage)
    return sub


def spread(row, height):
    return jnp.broadcast_to(row, (height, LANES))


def kernel(
    groups, subs, height, blocks, span, keep, relaxed,
    vel_any, prop_any, first_any, second_any, raw_any, target_any, live_any, imp_any,
    vel_out, imp_out,
    vel_ref, prop_ref, first_ref, second_ref, raw_ref, target_ref, live_ref, imp_ref,
    geo_ref, table, wide_parts, parts, onehot, low_s, chunk_s, jac, gain, imp, coef, rowbuf,
    acc, mail_out, mail_in, mass_out, mass_in, talk_out, talk_in, red_out, red_in,
    s_load, s_mail, r_mail, s_mass, r_mass, s_talk, r_talk, s_red, r_red,
):
    owner, sub = lax.axis_index("owner"), lax.axis_index("sub")
    rows = VEL * height
    every = (VEL + PROPS) * height
    owned = height * WIDE
    full = (groups - 1) // PAIRED
    head = groups - PAIRED * full
    mirrored = groups & (groups - 1) == 0

    def partner(k):
        if not mirrored:
            return lax.rem(owner + k, groups)
        q = owner
        for bit in range(groups.bit_length() - 1):
            step = 2**bit
            chosen = lax.rem(lax.div(k, step), 2) if not isinstance(k, int) else k // step % 2
            q = q + chosen * (step - 2 * step * lax.rem(lax.div(owner, step), 2))
        return q

    def there(k):
        return k if mirrored else lax.rem(groups - k, groups)

    barrier = pltpu.get_barrier_semaphore()

    def signal(k, carry):
        pl.semaphore_signal(
            barrier, inc=1, device_id=(partner(k), sub), device_id_type=MESH
        )
        return carry

    lax.fori_loop(1, groups, signal, 0)
    for j in range(1, subs):
        pl.semaphore_signal(
            barrier, inc=1, device_id=(owner, across(sub, j)), device_id_type=MESH
        )

    loads = [
        pltpu.make_async_copy(source, target, s_load.at[n])
        for n, (source, target) in enumerate(
            [
                (raw_any, raw_ref),
                (live_any, live_ref),
                (second_any, second_ref),
                (first_any, first_ref),
                (vel_any, vel_ref),
                (prop_any, prop_ref),
                (target_any, target_ref),
                (imp_any, imp_ref),
            ]
        )
    ]
    for load in loads:
        load.start()

    def link(source, target, send_sem, recv_sem):
        def outgoing(k, *at):
            return remote(
                source.at[(*at, k)], target.at[(*at, there(k))], send_sem.at[(*at, k)],
                recv_sem.at[(*at, there(k))], (partner(k), sub),
            )

        def incoming(k, *at):
            return remote(
                source.at[(*at, k)], target.at[(*at, k)], send_sem.at[(*at, k)],
                recv_sem.at[(*at, k)], (partner(k), sub),
            )

        return outgoing, incoming

    mail, mail_here = link(mail_out, mail_in, s_mail, r_mail)
    mass, mass_here = link(mass_out, mass_in, s_mass, r_mass)
    talk, talk_here = link(talk_out, talk_in, s_talk, r_talk)

    def part(b):
        return pl.ds(b * SUB, SUB)

    def over_blocks(body):
        if blocks == 1:
            body(0)
        else:
            def run(b, carry):
                body(b)
                return carry

            lax.fori_loop(0, blocks, run, 0)

    def far_first(body):
        def run(j, carry):
            body([groups - 1 - PAIRED * j - n for n in range(PAIRED)])
            return carry

        lax.fori_loop(0, full, run, 0)
        body(list(range(head - 1, -1, -1)))

    def near_first(body):
        def run(j, carry):
            body([head + PAIRED * j + n for n in range(PAIRED)])
            return carry

        body([0])
        body(list(range(1, head)))
        lax.fori_loop(0, full, run, 0)

    def here(k):
        return isinstance(k, int) and k == 0

    def live_of(q, b):
        lane = lax.broadcasted_iota(jnp.int32, (SUB, LANES), 1)
        line = lax.broadcasted_iota(jnp.int32, (SUB, LANES), 0)
        bound = jnp.zeros((SUB, LANES), jnp.int32)
        for i in range(SUB):
            row = (q * blocks + b) * SUB + i
            left = live_ref[row // span] - (row % span) * LANES
            bound = jnp.where(line == i, left, bound)
        return lane < bound

    def local(index):
        return index - lax.div(index, jnp.full_like(index, owned)) * owned

    def write_mail(k, carry):
        q = partner(k)

        def block(b):
            for r in range(9):
                for i in range(SUB):
                    start = pl.multiple_of(((q * blocks + b) * SUB + i) * LANES, LANES)
                    geo_ref[r, k, pl.ds(b * SUB + i, 1), :] = raw_ref[
                        pl.ds(r, 1), pl.ds(start, LANES)
                    ]
            normal = [geo_ref[r, k, part(b)] for r in range(3)]
            cross = cross_rows([geo_ref[6 + r, k, part(b)] for r in range(3)], normal)
            live = live_of(q, b)
            for r, value in enumerate(normal + cross):
                mail_out[k, r, part(b)] = jnp.where(live, -value, 0.0)
            mail_out[k, VEL, part(b)] = local(second_ref[q, part(b)]).astype(jnp.float32)

        over_blocks(block)
        return carry

    for load in loads[:3]:
        load.wait()
    lax.fori_loop(0, groups, write_mail, 0)
    for load in loads[3:]:
        load.wait()

    for r in range(VEL):
        for c in range(height):
            table[pl.ds(r * height + c, 1), :] = vel_ref[pl.ds(r, 1), pl.ds(c * WIDE, WIDE)]
    for r in range(PROPS):
        for c in range(height):
            rowbuf[pl.ds(r * height + c, 1), :] = prop_ref[pl.ds(r, 1), pl.ds(c * WIDE, WIDE)]
    whole = jnp.concatenate([table[...], rowbuf[...]], axis=0)
    whole_high = whole.astype(jnp.bfloat16)
    wide_parts[pl.ds(0, every), :] = whole_high
    wide_parts[pl.ds(every, every), :] = (whole - whole_high.astype(jnp.float32)).astype(
        jnp.bfloat16
    )

    def hot(low, i):
        tall = lax.broadcasted_iota(jnp.int32, (WIDE, LANES), 0)
        return jnp.where(tall == spread(low[i : i + 1], WIDE), 1.0, 0.0).astype(HOT)

    def hot_tile(side, k, b):
        if keep:
            return onehot[side, k, b]
        low = low_s[side, k, part(b)]
        return jnp.concatenate([hot(low, i) for i in range(SUB)], axis=1)

    def hits(chunk):
        tall = lax.broadcasted_iota(jnp.int32, (height, LANES), 0)
        return [tall == spread(chunk[i : i + 1], height) for i in range(SUB)]

    def picked(values, tile):
        half = values.shape[0] // 2
        out = lax.dot_general(
            values[...], tile, (((1,), (0,)), ((), ())), preferred_element_type=jnp.float32
        )
        return out[:half] + out[half:]

    def lookup(got, masks, lines):
        found = []
        for i in range(SUB):
            total = None
            for r, line in lines:
                piece = got[r * height : (r + 1) * height, i * LANES : (i + 1) * LANES]
                if line is not None:
                    piece = piece * spread(line(i), height)
                total = piece if total is None else total + piece
            found.append(jnp.sum(jnp.where(masks[i], total, 0.0), axis=0, keepdims=True))
        return jnp.concatenate(found, axis=0)

    def prepare(side, k, b, index, values, aim):
        low = lax.rem(index, jnp.full_like(index, WIDE))
        chunk = lax.div(index, jnp.full_like(index, WIDE))
        low_s[side, k, part(b)] = low
        chunk_s[side, k, part(b)] = chunk
        pieces = [hot(low, i) for i in range(SUB)]
        if keep:
            for i in range(SUB):
                onehot[side, k, b, :, pl.ds(i * LANES, LANES)] = pieces[i]
        got = picked(wide_parts, jnp.concatenate(pieces, axis=1))
        masks = hits(chunk)
        prop = [lookup(got, masks, [(VEL + r, None)]) for r in range(PROPS)]
        speed = lookup(
            got, masks, [(r, lambda i, r=r: values[r][i : i + 1]) for r in range(VEL)]
        )
        total = prop[0]
        for r in range(VEL):
            jac[side, k, r, part(b)] = values[r]
            gain[side, k, r, part(b)] = prop[max(0, r - 2)] * values[r]
        for r in range(3):
            total += values[3 + r] * values[3 + r] * prop[1 + r]
        mass_out[k, side, part(b)] = total
        mass_out[k, 3 + side, part(b)] = aim - speed

    def prepare_first(ks):
        def block(b):
            for k in ks:
                q = partner(k)
                normal = [geo_ref[r, k, part(b)] for r in range(3)]
                cross = cross_rows([geo_ref[3 + r, k, part(b)] for r in range(3)], normal)
                index = local(first_ref[q, part(b)])
                prepare(0, k, b, index, normal + cross, target_ref[q, part(b)])
                start = imp_ref[q, part(b)]
                imp[0, k, part(b)] = start
                mass_out[k, 2, part(b)] = start

        over_blocks(block)

    def prepare_second(ks):
        for k in ks:
            if not here(k):
                mail_here(k).wait_recv()

        def block(b):
            for k in ks:
                source = mail_out if here(k) else mail_in
                values = [source[k, r, part(b)] for r in range(VEL)]
                index = source[k, VEL, part(b)].astype(jnp.int32)
                prepare(1, k, b, index, values, 0.0)

        over_blocks(block)
        for k in ks:
            if not here(k):
                mass(k).start()

    def post(j, carry):
        mail(j).start()
        return carry

    far_first(prepare_first)
    pl.semaphore_wait(barrier, groups + subs - 2)
    lax.fori_loop(1, groups, post, 0)
    near_first(prepare_second)

    def speak(t):
        def some(ks):
            def block(b):
                for k, side in [(k, side) for k in ks for side in range(2)]:
                    got = picked(parts, hot_tile(side, k, b))
                    masks = hits(chunk_s[side, k, part(b)])
                    lines = [
                        (r, lambda i, r=r: jac[side, k, r, pl.ds(b * SUB + i, 1)])
                        for r in range(VEL)
                    ]
                    aim = target_ref[partner(k), part(b)] if side == 0 else 0.0
                    talk_out[t, k, side, part(b)] = aim - lookup(got, masks, lines)

            over_blocks(block)
            for k in ks:
                if not here(k):
                    talk(k, t).start()

        far_first(some)

    def place(deltas, side, k, b):
        coarse = [d.astype(jnp.bfloat16).astype(jnp.float32) for d in deltas]
        fine = [d - c for d, c in zip(deltas, coarse)]
        masks = hits(chunk_s[side, k, part(b)])
        left = []
        for i in range(SUB):
            lines = [
                jnp.where(masks[i], spread(x[i : i + 1], height), 0.0) for x in coarse + fine
            ]
            left.append(jnp.concatenate(lines, axis=0).astype(jnp.bfloat16))
        out = lax.dot_general(
            jnp.concatenate(left, axis=1),
            hot_tile(side, k, b),
            (((1,), (1,)), ((), ())),
            preferred_element_type=jnp.float32,
        )
        return out[:rows] + out[rows:]

    def settle(k, b):
        peer_ref = mass_out if here(k) else mass_in
        for side in range(2):
            value = relaxed / (mass_out[k, side, part(b)] + peer_ref[k, 1 - side, part(b)])
            if side == 0:
                value = jnp.where(live_of(partner(k), b), value, 0.0)
            coef[side, k, part(b)] = value
        imp[1, k, part(b)] = peer_ref[k, 2, part(b)]

    def act(t, first):
        acc[...] = jnp.zeros_like(acc)

        def some(ks):
            for k in ks:
                if not here(k):
                    if first:
                        mass_here(k).wait_recv()
                    else:
                        talk_here(k, t).wait_recv()

            def block(b):
                moved = []
                for k in ks:
                    if first:
                        settle(k, b)
                    if first:
                        mine_ref, peer_ref = mass_out, mass_out if here(k) else mass_in
                        at, shift = (k,), 3
                    else:
                        mine_ref, peer_ref = talk_out, talk_out if here(k) else talk_in
                        at, shift = (t, k), 0
                    for side in range(2):
                        push = (
                            mine_ref[(*at, shift + side, part(b))]
                            + peer_ref[(*at, shift + 1 - side, part(b))]
                        )
                        before = imp[side, k, part(b)]
                        fresh = jnp.maximum(before + push * coef[side, k, part(b)], 0.0)
                        imp[side, k, part(b)] = fresh
                        applied = fresh - before
                        deltas = [applied * gain[side, k, r, part(b)] for r in range(VEL)]
                        moved.append(place(deltas, side, k, b))
                acc[...] += functools.reduce(jnp.add, moved)

            over_blocks(block)

        near_first(some)

    def reduce(t, j):
        return remote(
            red_out.at[t], red_in.at[t, j], s_red.at[t, j], r_red.at[t, j],
            (owner, across(sub, j)),
        )

    def advance(t):
        red_out[t] = acc[...]
        for j in range(1, subs):
            reduce(t, j).start()
        terms = [acc[...]]
        for j in range(1, subs):
            reduce(t, j).wait_recv()
            terms.append(red_in[t, j])
        while len(terms) > 1:
            terms = [a + b for a, b in zip(terms[::2], terms[1::2])]
        value = table[...] + terms[0]
        table[...] = value
        high = value.astype(jnp.bfloat16)
        parts[pl.ds(0, rows), :] = high
        parts[pl.ds(rows, rows), :] = (value - high.astype(jnp.float32)).astype(jnp.bfloat16)

    act(0, True)
    advance(0)

    def iteration(t, carry):
        speak(t)
        act(t, False)
        advance(t)
        return carry

    lax.fori_loop(1, ITERS, iteration, 0)

    for r in range(VEL):
        for c in range(height):
            vel_out[pl.ds(r, 1), pl.ds(c * WIDE, WIDE)] = table[pl.ds(r * height + c, 1), :]

    def finish(k, carry):
        imp_out[partner(k)] = imp[0, k]
        return carry

    lax.fori_loop(0, groups, finish, 0)

    def sent(k, carry):
        mail(k).wait_send()
        mass(k).wait_send()
        for t in range(1, ITERS):
            talk(k, t).wait_send()
        return carry

    lax.fori_loop(1, groups, sent, 0)
    for t in range(ITERS):
        for j in range(1, subs):
            reduce(t, j).wait_send()


def on_device(
    groups, subs, velocity, properties, first_body, second_body, geometry, target_speed,
    warm_impulse, live_pairs
):
    owned = velocity.shape[1]
    height = owned // WIDE
    count = first_body.shape[0]
    rows = count // (groups * LANES)
    blocks = rows // SUB
    tiles = (groups, rows, LANES)
    keep = 2 * count * WIDE <= KEEP_BYTES
    kept = (2, groups, blocks, WIDE, SUB * LANES) if keep else (1, 1, 1, 32, LANES)
    span = count // live_pairs.shape[0] // LANES

    f32 = jnp.float32
    pair = (2, groups, rows, LANES)
    operands = (
        velocity,
        properties,
        first_body.reshape(tiles),
        second_body.reshape(tiles),
        geometry,
        target_speed.reshape(tiles),
        live_pairs,
        warm_impulse.reshape(tiles),
    )
    held = [pltpu.VMEM(x.shape, x.dtype) for x in operands]
    held[6] = pltpu.SMEM(live_pairs.shape, live_pairs.dtype)
    speeds, impulse = pl.pallas_call(
        functools.partial(kernel, groups, subs, height, blocks, span, keep, relax),
        name="contacts",
        out_shape=(
            pltpu.VMEM((VEL, owned), f32),
            pltpu.VMEM(tiles, f32),
        ),
        in_specs=[pl.BlockSpec(memory_space=pl.ANY)] * 8,
        out_specs=(pl.BlockSpec(memory_space=pltpu.VMEM),) * 2,
        scratch_shapes=held
        + [
            pltpu.VMEM((geometry.shape[0],) + tiles, f32),
            pltpu.VMEM((VEL * height, WIDE), f32),
            pltpu.VMEM((2 * (VEL + PROPS) * height, WIDE), jnp.bfloat16),
            pltpu.VMEM((2 * VEL * height, WIDE), jnp.bfloat16),
            pltpu.VMEM(kept, HOT),
            pltpu.VMEM(pair, jnp.int32),
            pltpu.VMEM(pair, jnp.int32),
            pltpu.VMEM((2, groups, VEL, rows, LANES), f32),
            pltpu.VMEM((2, groups, VEL, rows, LANES), f32),
            pltpu.VMEM(pair, f32),
            pltpu.VMEM(pair, f32),
            pltpu.VMEM((PROPS * height, WIDE), f32),
            pltpu.VMEM((VEL * height, WIDE), f32),
            pltpu.VMEM((groups, MAIL, rows, LANES), f32),
            pltpu.VMEM((groups, MAIL, rows, LANES), f32),
            pltpu.VMEM((groups, 5, rows, LANES), f32),
            pltpu.VMEM((groups, 5, rows, LANES), f32),
            pltpu.VMEM((ITERS, groups, 2, rows, LANES), f32),
            pltpu.VMEM((ITERS, groups, 2, rows, LANES), f32),
            pltpu.VMEM((ITERS, VEL * height, WIDE), f32),
            pltpu.VMEM((ITERS, subs, VEL * height, WIDE), f32),
            pltpu.SemaphoreType.DMA((len(operands),)),
        ]
        + [pltpu.SemaphoreType.DMA((groups,))] * 4
        + [pltpu.SemaphoreType.DMA((ITERS, groups))] * 2
        + [pltpu.SemaphoreType.DMA((ITERS, subs))] * 2,
        compiler_params=pltpu.CompilerParams(collective_id=0, has_side_effects=True),
    )(*operands)
    return (speeds, impulse.reshape(count))


def solution(mesh):
    groups, subs = mesh.shape["owner"], mesh.shape["sub"]
    return jax.shard_map(
        functools.partial(on_device, groups, subs),
        mesh=mesh,
        in_specs=(
            P(None, "owner"),
            P(None, "owner"),
            P(("owner", "sub")),
            P(("owner", "sub")),
            P(None, ("owner", "sub")),
            P(("owner", "sub")),
            P(("owner", "sub")),
            P(("owner", "sub")),
        ),
        out_specs=(P(None, "owner"), P(("owner", "sub"))),
        check_vma=False,
    )
```
